256 devices in a mesh: rep: 64 (over z, x, core), rows: 4 (over y).
Axes of the slice: x: 4, y: 4, z: 8, core: 2. Of those that a mesh axis runs over, the one named last changes fastest.
Arguments:
- pooled_grad: bfloat16 [262144, 2, 128], P(('rep', 'rows')), may hold values from -6 to 6
- slot_source: int32 [256, 4, 1024], P(('rep', 'rows')), may hold values from 0 to 2047, as said below
- slot_target: int32 [256, 4, 1024], P(('rep', 'rows')), may hold values from 0 to 8191, as said below
- slot_count: int32 [256, 4], P(('rep', 'rows')), may hold values from 128 to 1024, as said below
- table_rows: float32 [2, 16384, 128], P(None, 'rows'), may hold values from -1.5 to 1.5
- accum: float32 [2, 16384], P(None, 'rows'), may hold values from 0.01 to 1
Outputs:
- new_rows: float32 [2, 16384, 128], P(None, 'rows')
- new_accum: float32 [2, 16384], P(None, 'rows')
The draws below stay inside these ranges and needn't reach their ends.
Inputs may be any that keep to these rules, and one draw needn't show every extreme that they name: `slot_source`: entry q encodes a local sample q // 2 and a table q % 2; the table agrees with that of slot_target at the same slot. `slot_target`: entry t encodes a table t // 4096 and a row t % 4096 of the owner's shard; rows repeat across slots and senders. `slot_count`: slots at or past the count carry no lookup; every sender fills all slots to some owner.
All inputs are finite; a program needn't handle non-finite values.
Results may differ from the reference program's by a relative error of at most 0.0003.
Values may be sent and summed in bfloat16 or wider, within the bound.
No kernel may reach another device: no remote copies, remote signals or barrier semaphores. Data moves between devices by JAX's collectives and lax.ppermute only.
A program may use at most 64 MiB of HBM per device.

```python
import math
import jax
import jax.numpy as jnp
from jax import lax

W = 128
ROWS_DEV = 4096
TABLES = 2
SAMP_DEV = 1024
OWNERS = 4
SENDERS = 256
ROWS = 16384
SAMPLES = 262144
CAP = 1024


def layout(key):
    folded = jax.random.fold_in(key, 4242)
    subkeys = jax.random.split(folded, 8)
    owner_ids = jnp.arange(OWNERS, dtype=jnp.int32)
    shape = (SENDERS, OWNERS, CAP)
    sample = jax.random.randint(subkeys[2], shape, 0, SAMP_DEV, dtype=jnp.int32)
    table_ids = jax.random.randint(subkeys[3], shape, 0, TABLES, dtype=jnp.int32)
    hot_count = ROWS_DEV // 16
    hot_rows = jax.random.randint(subkeys[4], (OWNERS, TABLES, hot_count), 0, ROWS_DEV, dtype=jnp.int32)
    pick_hot = jax.random.randint(subkeys[5], shape, 0, 4, dtype=jnp.int32) == 0
    hot_pick = jax.random.randint(subkeys[6], shape, 0, hot_count, dtype=jnp.int32)
    cold_rows = jax.random.randint(subkeys[7], shape, 0, ROWS_DEV, dtype=jnp.int32)
    owner_grid = jnp.broadcast_to(owner_ids[None, :, None], shape)
    chosen_hot = hot_rows[owner_grid, table_ids, hot_pick]
    row_ids = jnp.where(pick_hot, chosen_hot, cold_rows).astype(jnp.int32)
    source = (sample * TABLES + table_ids).astype(jnp.int32)
    target = (table_ids * ROWS_DEV + row_ids).astype(jnp.int32)
    return (source, target)


def draw_slot_source(key, part):
    return layout(key)[0]


def draw_slot_target(key, part):
    return layout(key)[1]


def draw_slot_count(key, part):
    folded = jax.random.fold_in(key, 9191)
    first_key, second_key = jax.random.split(folded, 2)
    owner_ids = jnp.arange(OWNERS, dtype=jnp.int32)
    busy_owner = jax.random.randint(first_key, (SENDERS,), 0, OWNERS, dtype=jnp.int32)
    spread = jax.random.randint(second_key, (SENDERS, OWNERS), CAP // 8, CAP + 1, dtype=jnp.int32)
    is_busy = owner_ids[None, :] == busy_owner[:, None]
    return jnp.where(is_busy, CAP, spread).astype(jnp.int32)


def block_scale(key, dims, shards, smallest, high):
    def one(axis_at, blocks):
        heights = jax.random.uniform(jax.random.fold_in(jax.random.fold_in(key, 6), axis_at), (blocks,), jnp.float32, smallest / len(shards), high / len(shards))
        return jnp.repeat(jnp.exp(heights), dims[axis_at] // blocks).reshape((-1,) + (1,) * (len(dims) - axis_at - 1))

    gain = one(*shards[0])
    for cut in shards[1:]:
        gain = gain * one(*cut)
    return gain


def centred(key, dims, scale, limit, pieces=(), kind=jnp.bfloat16):
    gain = block_scale(key, dims, pieces, -0.22, 0.18) if pieces else 1.0
    result = jax.random.normal(key, dims, jnp.float32) * scale * gain
    return jnp.minimum(jnp.maximum(result, -limit), limit).astype(kind)


def setup_inputs(seed: int = 0) -> dict:
    arg_keys = jax.random.split(jax.random.key(seed), 7)
    pooled_grad = centred(arg_keys[0], (SAMPLES, TABLES, W), 1.0, 6.0, ((0, 256),))
    slot_source = draw_slot_source(jax.random.fold_in(arg_keys[6], 71), 0)
    slot_target = draw_slot_target(jax.random.fold_in(arg_keys[6], 71), 0)
    slot_count = draw_slot_count(jax.random.fold_in(arg_keys[6], 71), 0)
    table_rows = centred(arg_keys[4], (TABLES, ROWS, W), 0.1, 1.5, ((1, 4),), jnp.float32)
    accum = jnp.clip(jnp.exp(math.log(1.0) - 4.6051702 * jax.random.uniform(arg_keys[5], (TABLES, ROWS), jnp.float32) ** block_scale(arg_keys[5], (TABLES, ROWS), ((1, 4),), -0.2, 0.2)), 0.01, 1.0)
    return {"pooled_grad": pooled_grad, "slot_source": slot_source, "slot_target": slot_target, "slot_count": slot_count, "table_rows": table_rows, "accum": accum}


LEARN_RATE = 0.1
EPSILON = 1e-06

def reference(pooled_grad, slot_source, slot_target, slot_count, table_rows, accum):
    flat_grad = pooled_grad.reshape(SENDERS * SAMP_DEV * TABLES, W)
    slot_ids = jnp.arange(CAP, dtype=jnp.int32)
    owner_ids = jnp.arange(OWNERS, dtype=jnp.int32)

    def add_sender(summed, inputs):
        sender, source, target, counts = inputs
        filled = slot_ids[None, :] < counts[:, None]
        picked = flat_grad[sender * (SAMP_DEV * TABLES) + source].astype(jnp.float32)
        picked = jnp.where(filled[:, :, None], picked, jnp.zeros_like(picked))
        table_ids = target // ROWS_DEV
        row_ids = target % ROWS_DEV
        segment = table_ids * ROWS + owner_ids[:, None] * ROWS_DEV + row_ids
        summed = summed.at[segment.reshape(-1)].add(picked.reshape(-1, W))
        return (summed, None)
    start = jnp.zeros((TABLES * ROWS, W), jnp.float32)
    senders = jnp.arange(SENDERS, dtype=jnp.int32)
    summed, _ = lax.scan(add_sender, start, (senders, slot_source, slot_target, slot_count))
    row_grad = summed.reshape(TABLES, ROWS, W)
    new_accum = accum + lax.optimization_barrier(jnp.mean(row_grad * row_grad, axis=2))
    new_rows = table_rows - LEARN_RATE * row_grad / (jnp.sqrt(new_accum)[:, :, None] + EPSILON)
    return (new_rows, new_accum)
```

```python
import functools

import jax
import jax.numpy as jnp
from jax import lax
from jax.experimental import pallas as pl
from jax.experimental.pallas import tpu as pltpu
from jax.sharding import Mesh
from jax.sharding import PartitionSpec as P

REP_ROWS = ("rep_0", "rep_1", "rep_2", "rows")
PLANE = ("rep_0", "rep_1")

LEARN_RATE = 0.1
EPSILON = 1e-06
LANES = 128
SPARE = 8
STEPS = 64.0
TOP = 32700.0
TINY = 1e-30

VM = pl.BlockSpec(memory_space=pltpu.VMEM)
SM = pl.BlockSpec(memory_space=pltpu.SMEM)


def pick_kernel(unroll, keys, flat, out, wide, stage):
    owners, cap, _ = out.shape
    wide[...] = flat[...].astype(jnp.float32)
    for owner in range(owners):
        slot = owner % 2

        def body(step, carry):
            first = step * unroll
            for u in range(unroll):
                key = keys[owner * cap + first + u]
                stage[slot, pl.ds(first + u, 1), :] = wide[pl.ds(key, 1), :]
            return carry

        lax.fori_loop(0, cap // unroll, body, 0)
        out[owner] = stage[slot].astype(jnp.bfloat16)


def pick_rows(keys, flat, owners):
    cap = keys.shape[0] // owners
    width = flat.shape[1]
    return pl.pallas_call(
        functools.partial(pick_kernel, 32),
        out_shape=jax.ShapeDtypeStruct((owners, cap, width), jnp.bfloat16),
        in_specs=[SM, VM],
        out_specs=VM,
        scratch_shapes=[
            pltpu.VMEM(flat.shape, jnp.float32),
            pltpu.VMEM((2, cap, width), jnp.float32),
        ],
        cost_estimate=pl.CostEstimate(flops=10**8, bytes_accessed=2 * 10**6, transcendentals=0),
        name="pick",
    )(keys, flat)


def scatter_kernel(unroll, core, keys, grads, mine, other, *scratch):
    senders, cap, _ = grads.shape
    sums, wides = scratch[:senders], scratch[senders:]
    half = mine.shape[0]
    for k in range(senders):
        wides[k][...] = grads[k].astype(jnp.float32)
        sums[k][...] = jnp.zeros(sums[k].shape, jnp.float32)

    def body(step, carry):
        first = step * unroll
        for u in range(unroll):
            for k in range(senders):
                key = keys[k * cap + first + u]
                sums[k][pl.ds(key, 1), :] += wides[k][pl.ds(first + u, 1), :]
        return carry

    lax.fori_loop(0, cap // unroll, body, 0)
    for out, index in ((mine, core[0]), (other, 1 - core[0])):
        base = pl.multiple_of(index * half, half)
        total = sums[0][pl.ds(base, half), :]
        for part in sums[1:]:
            total = total + part[pl.ds(base, half), :]
        out[...] = total


def scatter_add(core, keys, grads, rows):
    senders, cap, width = grads.shape
    shape = jax.ShapeDtypeStruct((rows // 2, width), jnp.float32)
    return pl.pallas_call(
        functools.partial(scatter_kernel, 4),
        out_shape=(shape, shape),
        in_specs=[SM, SM, VM],
        out_specs=(VM, VM),
        scratch_shapes=[pltpu.VMEM((rows + SPARE, width), jnp.float32)] * senders
        + [pltpu.VMEM((cap, width), jnp.float32)] * senders,
        compiler_params=pltpu.CompilerParams(vmem_limit_bytes=60 * 2**20),
        cost_estimate=pl.CostEstimate(flops=10**8, bytes_accessed=5 * 10**6, transcendentals=0),
        name="scatter",
    )(core, keys, grads)


def diagonal():
    shape = (LANES, LANES)
    return lax.broadcasted_iota(jnp.int32, shape, 0) == lax.broadcasted_iota(jnp.int32, shape, 1)


def to_row(column, diag):
    return jnp.sum(jnp.where(diag, column, 0.0), axis=0, keepdims=True)


def to_column(row, diag):
    return jnp.sum(jnp.where(diag, row, 0.0), axis=1, keepdims=True)


def encode(block, diag):
    peak = to_row(jnp.max(jnp.abs(block), axis=1, keepdims=True), diag)
    power = jnp.ceil(STEPS * jnp.log2(jnp.maximum(peak, TINY) / TOP))
    shrink = to_column(jnp.exp2(power * (-1.0 / STEPS)), diag)
    code = jnp.round(block * shrink).astype(jnp.int32).astype(jnp.int16)
    tail = jnp.broadcast_to(power, (SPARE, LANES)).astype(jnp.int32).astype(jnp.int16)
    return code, tail


def scale_row(tail):
    return jnp.exp2(tail.astype(jnp.int32).astype(jnp.float32)[0:1] * (1.0 / STEPS))


def encode_kernel(mine, got, out):
    diag = diagonal()

    def body(b, carry):
        rows = pl.ds(pl.multiple_of(b * LANES, LANES), LANES)
        code, tail = encode(mine[rows, :] + got[rows, :], diag)
        out[b, 0:LANES, :] = code
        out[b, LANES : LANES + SPARE, :] = tail
        return carry

    lax.fori_loop(0, out.shape[0], body, 0)


def encode_sum(mine, got):
    blocks = mine.shape[0] // LANES
    return pl.pallas_call(
        encode_kernel,
        out_shape=jax.ShapeDtypeStruct((blocks, LANES + SPARE, LANES), jnp.int16),
        in_specs=[VM, VM],
        out_specs=VM,
        name="encode",
    )(mine, got)


def reduce_kernel(parts, out):
    diag = diagonal()

    def body(j, total):
        scale = to_column(scale_row(parts[j, LANES : LANES + SPARE, :]), diag)
        return total + parts[j, 0:LANES, :].astype(jnp.int32).astype(jnp.float32) * scale

    total = lax.fori_loop(0, parts.shape[0], body, jnp.zeros((LANES, LANES), jnp.float32))
    code, tail = encode(total, diag)
    out[0:LANES, :] = code
    out[LANES : LANES + SPARE, :] = tail


def reduce_parts(parts):
    return pl.pallas_call(
        reduce_kernel,
        out_shape=jax.ShapeDtypeStruct(parts.shape[1:], jnp.int16),
        in_specs=[VM],
        out_specs=VM,
        name="reduce",
    )(parts)


def update_kernel(blocks, core, mine, got, rows, state, new_rows, new_state):
    diag = diagonal()
    base = pl.program_id(0) * blocks
    for table in range(2):
        own = core[0] == table
        for k in range(blocks):
            pair = [ref[base + k].astype(jnp.int32) for ref in (mine, got)]
            data = jnp.where(own, pair[0], pair[1]).astype(jnp.float32)
            code = data[0:LANES]
            scale = jnp.exp2(data[LANES : LANES + 1] * (1.0 / STEPS))
            squares = to_row(jnp.sum(code * code, axis=1, keepdims=True), diag)
            lanes = pl.ds(k * LANES, LANES)
            updated = state[pl.ds(table, 1), lanes] + squares * (scale * scale) * (1.0 / LANES)
            new_state[pl.ds(table, 1), lanes] = updated
            factor = to_column(LEARN_RATE * scale / (jnp.sqrt(updated) + EPSILON), diag)
            new_rows[table, lanes, :] = rows[table, lanes, :] - code * factor


def update(core, mine, got, rows, state):
    tables, rows_dev, width = rows.shape
    blocks = 4
    size = blocks * LANES
    row_spec = pl.BlockSpec((tables, size, width), lambda i: (0, i, 0))
    state_spec = pl.BlockSpec((tables, size), lambda i: (0, i))
    return pl.pallas_call(
        functools.partial(update_kernel, blocks),
        grid=(rows_dev // size,),
        out_shape=(
            jax.ShapeDtypeStruct(rows.shape, jnp.float32),
            jax.ShapeDtypeStruct(state.shape, jnp.float32),
        ),
        in_specs=[SM, VM, VM, row_spec, state_spec],
        out_specs=(row_spec, state_spec),
        name="update",
    )(core, mine, got, rows, state)


def swap_cores(x):
    return lax.ppermute(x, "rep_2", [(0, 1), (1, 0)])


def shards(pooled_grad, slot_source, slot_target, slot_count, table_rows, accum):
    feature = pooled_grad.shape[2]
    tables, rows_dev, _ = table_rows.shape
    owners, cap = slot_source.shape[1:]
    row_total = tables * rows_dev
    core = lax.axis_index("rep_2").astype(jnp.int32).reshape(1)
    flat_grad = pooled_grad.reshape(-1, feature)
    filled = jnp.arange(cap, dtype=jnp.int32)[None, :] < slot_count[0][:, None]
    targets = jnp.where(filled, slot_target[0], row_total)
    got_targets = lax.all_to_all(targets, "rows", 0, 0, tiled=True)
    picked = pick_rows(slot_source[0].reshape(-1), flat_grad, owners)
    got_grads = lax.all_to_all(picked, "rows", 0, 0, tiled=True)
    mine, other = scatter_add(core, got_targets.reshape(-1), got_grads, row_total)
    coded = encode_sum(mine, swap_cores(other))
    own = reduce_parts(lax.all_to_all(coded, PLANE, 0, 0, tiled=True))
    spread = jnp.broadcast_to(own[None], coded.shape)
    whole = lax.all_to_all(spread, PLANE, 0, 0, tiled=True)
    return update(core, whole, swap_cores(whole), table_rows, accum)


def solution(mesh):
    split = Mesh(
        mesh.devices.reshape(8, 4, 2, mesh.shape["rows"]), ("rep_0", "rep_1", "rep_2", "rows")
    )
    placed = (
        P(REP_ROWS, None, None),
        P(REP_ROWS, None, None),
        P(REP_ROWS, None, None),
        P(REP_ROWS, None),
        P(None, "rows", None),
        P(None, "rows"),
    )
    return jax.shard_map(
        shards,
        mesh=split,
        in_specs=placed,
        out_specs=(P(None, "rows", None), P(None, "rows")),
        check_vma=False,
    )
```

```python
import functools

import jax
import jax.numpy as jnp
from jax import lax
from jax.experimental import pallas as pl
from jax.experimental.pallas import tpu as pltpu
from jax.sharding import Mesh
from jax.sharding import PartitionSpec as P


AXES = ("far", "pair", "ring", "core", "rows")

LEARN_RATE = 0.1
EPSILON = 1e-06
LANES = 128
SPARE = 8
CODED = LANES + SPARE
STEPS = 64.0
TOP = 32700.0
TINY = 1e-30
ROUNDER = 12582912.0

VM = pl.BlockSpec(memory_space=pltpu.VMEM)
SM = pl.BlockSpec(memory_space=pltpu.SMEM)


def cost(flops):
    return pl.CostEstimate(flops=flops, bytes_accessed=10**6, transcendentals=0)


def pick_kernel(unroll, cap, owners, keys, flat, *refs):
    count = len(refs) // 2
    wide, stages = refs[-1], refs[count : 2 * count]
    wide[...] = flat[...].astype(jnp.float32)
    for which in range(count):
        out, stage = refs[which], stages[which]
        base = owners[which] * cap

        def body(step, carry):
            first = step * unroll
            for u in range(unroll):
                key = keys[base + first + u]
                stage[pl.ds(first + u, 1), :] = wide[pl.ds(key, 1), :]
            return carry

        lax.fori_loop(0, cap // unroll, body, 0)
        out[...] = stage[...].astype(jnp.bfloat16)


def pick_rows(owners, keys, flat, cap):
    count = owners.shape[0]
    width = flat.shape[1]
    shape = jax.ShapeDtypeStruct((cap, width), jnp.bfloat16)
    return pl.pallas_call(
        functools.partial(pick_kernel, 32, cap),
        out_shape=(shape,) * count,
        in_specs=[SM, SM, VM],
        out_specs=(VM,) * count,
        scratch_shapes=[pltpu.VMEM((cap, width), jnp.float32)] * count
        + [pltpu.VMEM(flat.shape, jnp.float32)],
        cost_estimate=cost(10**7 * count),
        name="pick",
    )(owners, keys, flat)


def scatter_kernel(unroll, senders, core, origins, keys, *refs):
    grads, (mine, other) = refs[:senders], refs[senders : senders + 2]
    sums, wides = refs[senders + 2 : 2 * senders + 2], refs[2 * senders + 2 :]
    cap = grads[0].shape[0]
    half = mine.shape[0]
    for k in range(senders):
        wides[k][...] = grads[k][...].astype(jnp.float32)
        sums[k][...] = jnp.zeros(sums[k].shape, jnp.float32)
    bases = [origins[k] * cap for k in range(senders)]

    def body(step, carry):
        first = step * unroll
        for u in range(unroll):
            for k in range(senders):
                key = keys[bases[k] + first + u]
                sums[k][pl.ds(key, 1), :] += wides[k][pl.ds(first + u, 1), :]
        return carry

    lax.fori_loop(0, cap // unroll, body, 0)
    for out, index in ((other, 1 - core[0]), (mine, core[0])):
        base = pl.multiple_of(index * half, half)
        total = sums[0][pl.ds(base, half), :]
        for part in sums[1:]:
            total = total + part[pl.ds(base, half), :]
        out[...] = total


def scatter_add(core, origins, keys, grads, rows):
    senders = len(grads)
    cap, width = grads[0].shape
    shape = jax.ShapeDtypeStruct((rows // 2, width), jnp.float32)
    return pl.pallas_call(
        functools.partial(scatter_kernel, 4, senders),
        out_shape=(shape, shape),
        in_specs=[SM, SM, SM] + [VM] * senders,
        out_specs=(VM, VM),
        scratch_shapes=[pltpu.VMEM((rows + SPARE, width), jnp.float32)] * senders
        + [pltpu.VMEM((cap, width), jnp.float32)] * senders,
        compiler_params=pltpu.CompilerParams(vmem_limit_bytes=40 * 2**20),
        cost_estimate=cost(10**8),
        name="scatter",
    )(core, origins, keys, *grads)


def diagonal():
    shape = (LANES, LANES)
    return lax.broadcasted_iota(jnp.int32, shape, 0) == lax.broadcasted_iota(jnp.int32, shape, 1)


def to_row(column, diag):
    return jnp.sum(jnp.where(diag, column, 0.0), axis=0, keepdims=True)


def to_column(row, diag):
    return jnp.sum(jnp.where(diag, row, 0.0), axis=1, keepdims=True)


def encode(block, diag):
    peak = to_row(jnp.max(jnp.abs(block), axis=1, keepdims=True), diag)
    power = jnp.ceil(STEPS * jnp.log2(jnp.maximum(peak, TINY) / TOP))
    shrink = to_column(jnp.exp2(power * (-1.0 / STEPS)), diag)
    whole = (block * shrink + ROUNDER) - ROUNDER
    tail = jnp.broadcast_to(power, (SPARE, LANES))
    return whole.astype(jnp.int32).astype(jnp.int16), tail.astype(jnp.int32).astype(jnp.int16)


def scale_row(tail):
    return jnp.exp2(tail.astype(jnp.int32).astype(jnp.float32)[0:1] * (1.0 / STEPS))


def decode(part, diag):
    scale = to_column(scale_row(part[LANES:CODED]), diag)
    return part[0:LANES].astype(jnp.int32).astype(jnp.float32) * scale


def encode_kernel(blocks, groups, mine, got, *outs):
    diag = diagonal()
    for d, out in enumerate(outs):
        for k in range(blocks):
            first = groups[d] * (blocks * LANES) + k * LANES
            rows = pl.ds(pl.multiple_of(first, LANES), LANES)
            out[k, 0:LANES, :], out[k, LANES:CODED, :] = encode(mine[rows, :] + got[rows, :], diag)


def encode_sum(groups, mine, got):
    count = groups.shape[0]
    blocks = mine.shape[0] // (LANES * count)
    shape = jax.ShapeDtypeStruct((blocks, CODED, LANES), jnp.int16)
    return pl.pallas_call(
        functools.partial(encode_kernel, blocks),
        out_shape=(shape,) * count,
        in_specs=[SM, VM, VM],
        out_specs=(VM,) * count,
        cost_estimate=cost(10**7),
        name="encode",
    )(groups, mine, got)


def first_sum_kernel(count, places, *refs):
    diag = diagonal()
    parts, outs = refs[:count], refs[count:]
    for out, k in zip(outs, [places[i] for i in range(len(outs))]):
        total = decode(parts[0][k], diag)
        for part in parts[1:]:
            total = total + decode(part[k], diag)
        out[0:LANES, :], out[LANES:CODED, :] = encode(total, diag)


def first_sum(places, parts):
    shape = jax.ShapeDtypeStruct((CODED, LANES), jnp.int16)
    blocks = parts[0].shape[0]
    return pl.pallas_call(
        functools.partial(first_sum_kernel, len(parts)),
        out_shape=(shape,) * blocks,
        in_specs=[SM] + [VM] * len(parts),
        out_specs=(VM,) * blocks,
        cost_estimate=cost(10**7),
        name="first_sum",
    )(places, *parts)


def last_sum_kernel(*refs):
    diag = diagonal()
    out = refs[-1]
    total = decode(refs[0][...], diag)
    for part in refs[1:-1]:
        total = total + decode(part[...], diag)
    out[0:LANES, :], out[LANES:CODED, :] = encode(total, diag)


def last_sum(parts):
    return pl.pallas_call(
        last_sum_kernel,
        out_shape=jax.ShapeDtypeStruct((CODED, LANES), jnp.int16),
        in_specs=[VM] * len(parts),
        out_specs=VM,
        cost_estimate=cost(10**6),
        name="last_sum",
    )(*parts)


def update_kernel(count, groups, core, places, *refs):
    mine, got = refs[:count], refs[count : 2 * count]
    rows, state, new_rows, new_state, held = refs[2 * count :]
    step = pl.program_id(0)
    for d in range(count):

        @pl.when(step == d)
        def _():
            held[core[0]] = mine[d][...]
            held[1 - core[0]] = got[d][...]

    diag = diagonal()
    for table in range(2):
        for k in range(held.shape[1]):
            data = held[table, k]
            code = data[0:LANES].astype(jnp.int32).astype(jnp.float32)
            scale = scale_row(data[LANES:CODED])
            squares = to_row(jnp.sum(code * code, axis=1, keepdims=True), diag)
            lanes = pl.ds(pl.multiple_of(places[k] * LANES, LANES), LANES)
            updated = state[pl.ds(table, 1), lanes] + squares * (scale * scale) * (1.0 / LANES)
            new_state[pl.ds(table, 1), lanes] = updated
            factor = to_column(LEARN_RATE * scale / (jnp.sqrt(updated) + EPSILON), diag)
            new_rows[table, lanes, :] = rows[table, lanes, :] - code * factor


def update(groups, core, places, mine, got, rows, state):
    tables, rows_dev, width = rows.shape
    count = len(mine)
    size = rows_dev // count
    row_spec = pl.BlockSpec((tables, size, width), lambda i, g, *_: (0, g[i], 0))
    state_spec = pl.BlockSpec((tables, size), lambda i, g, *_: (0, g[i]))
    return pl.pallas_call(
        functools.partial(update_kernel, count),
        grid_spec=pltpu.PrefetchScalarGridSpec(
            num_scalar_prefetch=3,
            grid=(count,),
            in_specs=[VM] * (2 * count) + [row_spec, state_spec],
            out_specs=(row_spec, state_spec),
            scratch_shapes=[pltpu.VMEM((2, *mine[0].shape), jnp.int16)],
        ),
        out_shape=(
            jax.ShapeDtypeStruct(rows.shape, jnp.float32),
            jax.ShapeDtypeStruct(state.shape, jnp.float32),
        ),
        cost_estimate=cost(10**7),
        name="update",
    )(groups, core, places, *mine, *got, rows, state)


def shift(x, axis, by):
    count = lax.axis_size(axis)
    return lax.ppermute(x, axis, [(i, (i + by) % count) for i in range(count)])


def square_shift(x, pair_by, ring_by):
    pairs, rings = lax.axis_size("pair"), lax.axis_size("ring")
    links = [
        (p * rings + r, (p + pair_by) % pairs * rings + (r + ring_by) % rings)
        for p in range(pairs)
        for r in range(rings)
    ]
    return lax.ppermute(x, ("pair", "ring"), links)


def shards(pooled_grad, slot_source, slot_target, slot_count, table_rows, accum):
    feature = pooled_grad.shape[2]
    tables, rows_dev, _ = table_rows.shape
    owners, cap = slot_source.shape[1:]
    row_total = tables * rows_dev
    far, pair, ring, core, row = (lax.axis_index(a).astype(jnp.int32) for a in AXES)
    fars, pairs, rings = (lax.axis_size(a) for a in AXES[:3])
    core = core.reshape(1)
    flat_grad = pooled_grad.reshape(-1, feature)
    filled = jnp.arange(cap, dtype=jnp.int32)[None, :] < slot_count[0][:, None]
    targets = jnp.where(filled, slot_target[0], row_total)
    got_targets = lax.all_to_all(targets, "rows", 0, 0, tiled=True)

    keys = slot_source[0].reshape(-1)
    grads = [None] * owners
    for group in ((2,), (1, 3), (0,)):
        hops = jnp.array(group, jnp.int32)
        picked = pick_rows((row + hops) % owners, keys, flat_grad, cap)
        for hop, block in zip(group, picked):
            grads[hop] = shift(block, "rows", hop) if hop else block
    origins = (row + owners - jnp.arange(owners, dtype=jnp.int32)) % owners
    mine, other = scatter_add(core, origins, got_targets.reshape(-1), grads, row_total)

    hops = [(p, r) for p in range(pairs) for r in (2, 1, 3, 0)]
    hops = hops[::-1]
    ahead = jnp.stack([(pair + p) % pairs * rings + (ring + r) % rings for p, r in hops])
    behind = jnp.stack([(pair - p) % pairs * rings + (ring - r) % rings for p, r in hops])
    far_hops = jnp.arange(fars, dtype=jnp.int32)
    coded = encode_sum(ahead, mine, shift(other, "core", 1))
    parts = [square_shift(c, *h) if h != (0, 0) else c for c, h in zip(coded, hops)]
    sums = first_sum((far + far_hops) % fars, parts)
    own = last_sum([shift(s, "far", f) if f else s for f, s in enumerate(sums)])
    bundle = jnp.stack([shift(own, "far", f) if f else own for f in range(fars)])
    whole = [square_shift(bundle, *h) if h != (0, 0) else bundle for h in hops]
    swapped = [shift(w, "core", 1) for w in whole]
    places = (far + fars - far_hops) % fars
    return update(behind, core, places, whole, swapped, table_rows, accum)


def solution(mesh):
    split = Mesh(mesh.devices.reshape(4, 2, 4, 2, mesh.shape["rows"]), AXES)
    placed = (
        P(AXES, None, None),
        P(AXES, None, None),
        P(AXES, None, None),
        P(AXES, None),
        P(None, "rows", None),
        P(None, "rows"),
    )
    return jax.shard_map(
        shards,
        mesh=split,
        in_specs=placed,
        out_specs=(P(None, "rows", None), P(None, "rows")),
        check_vma=False,
    )
```

```python
import functools

import jax
import jax.numpy as jnp
from jax import lax
from jax.experimental import pallas as pl
from jax.experimental.pallas import tpu as pltpu
from jax.sharding import Mesh
from jax.sharding import PartitionSpec as P


AXES = ("far", "pair", "ring", "core", "rows")
SQUARE = ("pair", "ring")
WAVES = 1

LEARN_RATE = 0.1
EPSILON = 1e-06
LANES = 128
SPARE = 8
CODED = LANES + SPARE
STEPS = 64.0
TOP = 32700.0
TINY = 1e-30
ROUNDER = 12582912.0

VM = pl.BlockSpec(memory_space=pltpu.VMEM)
SM = pl.BlockSpec(memory_space=pltpu.SMEM)


def room(mib):
    return pltpu.CompilerParams(vmem_limit_bytes=mib * 2**20)


def cost(flops):
    return pl.CostEstimate(flops=flops, bytes_accessed=10**6, transcendentals=0)


def pick_kernel(hops, cap, total, place, count, keys, targets, flat, *refs):
    outs, stages = refs[: len(hops)], refs[len(hops) : 2 * len(hops)]
    wide, held = refs[2 * len(hops) :]
    chunks, owners, _ = targets.shape
    unused = total
    slots = lax.broadcasted_iota(jnp.int32, (chunks, LANES), 0) * LANES
    slots = slots + lax.broadcasted_iota(jnp.int32, (chunks, LANES), 1)
    for owner in range(owners):
        held[owner] = jnp.where(slots < count[0, owner], targets[:, owner, :], unused)
    piece = 128

    def widen(step, carry):
        rows = pl.ds(pl.multiple_of(step * piece, piece), piece)
        wide[rows, :] = flat[rows, :].astype(jnp.float32)
        return carry

    lax.fori_loop(0, flat.shape[0] // piece, widen, 0)
    for hop, out, stage in zip(hops, outs, stages):
        owner = lax.rem(place[0] + hop, owners)

        def body(chunk, carry):
            first = chunk * LANES
            for u in range(LANES):
                key = keys[chunk, owner, u]
                stage[pl.ds(first + u, 1), :] = wide[pl.ds(key, 1), :]
            return carry

        lax.fori_loop(0, chunks, body, 0)

        def narrow(step, carry):
            rows = pl.ds(pl.multiple_of(step * piece, piece), piece)
            out[rows, :] = stage[rows, :].astype(jnp.bfloat16)
            return carry

        lax.fori_loop(0, cap // piece, narrow, 0)
        target = held[owner]
        upper = target >> 7
        out[cap : cap + SPARE, :] = upper.astype(jnp.float32).astype(jnp.bfloat16)
        lower = target - upper * LANES
        out[cap + SPARE : cap + 2 * SPARE, :] = lower.astype(jnp.float32).astype(jnp.bfloat16)


def pick_rows(hops, total, place, count, keys, targets, flat):
    chunks, owners, _ = keys.shape
    cap = chunks * LANES
    width = flat.shape[1]
    shape = jax.ShapeDtypeStruct((cap + 2 * SPARE, width), jnp.bfloat16)
    return pl.pallas_call(
        functools.partial(pick_kernel, hops, cap, total),
        out_shape=(shape,) * len(hops),
        in_specs=[SM, SM, SM, VM, VM],
        out_specs=(VM,) * len(hops),
        scratch_shapes=[pltpu.VMEM((cap, width), jnp.float32)] * len(hops)
        + [
            pltpu.VMEM(flat.shape, jnp.float32),
            pltpu.VMEM((owners, chunks, LANES), jnp.int32),
        ],
        cost_estimate=cost(10**7 * len(hops)),
        compiler_params=room(12),
        name="pick",
    )(place, count, keys, targets, flat)


def scatter_kernel(senders, cap, place, *refs):
    grads = refs[:senders]
    outs = refs[senders : senders + 2 * WAVES]
    refs = refs[senders + 2 * WAVES :]
    sums, wides = refs[:senders], refs[senders : 2 * senders]
    found, keys, sem = refs[2 * senders :]
    chunks = cap // LANES
    size = outs[0].shape[0]
    for k in range(senders):
        upper = grads[k][cap : cap + SPARE, :].astype(jnp.float32)
        lower = grads[k][cap + SPARE : cap + 2 * SPARE, :].astype(jnp.float32)
        found[k * chunks : (k + 1) * chunks, :] = (upper * LANES + lower).astype(jnp.int32)
    copy = pltpu.make_async_copy(found, keys, sem)
    copy.start()
    piece = 64

    def widen(step, carry):
        rows = pl.ds(pl.multiple_of(step * piece, piece), piece)
        for k in range(senders):
            wides[k][rows, :] = grads[k][rows, :].astype(jnp.float32)
        return carry

    def clear(step, carry):
        rows = pl.ds(pl.multiple_of(step * piece, piece), piece)
        for k in range(senders):
            sums[k][rows, :] = jnp.zeros((piece, LANES), jnp.float32)
        return carry

    lax.fori_loop(0, cap // piece, widen, 0)
    lax.fori_loop(0, sums[0].shape[0] // piece, clear, 0)
    copy.wait()

    def body(chunk, carry):
        first = chunk * LANES
        for u in range(LANES):
            for k in range(senders):
                key = keys[k * chunks + chunk, u]
                sums[k][pl.ds(key, 1), :] += wides[k][pl.ds(first + u, 1), :]
        return carry

    lax.fori_loop(0, chunks, body, 0)
    for which, index in ((1, 1 - place[1]), (0, place[1])):
        for wave in range(WAVES):
            base = pl.multiple_of((index * WAVES + wave) * size, size)
            out = outs[which * WAVES + wave]

            def add_up(step, carry):
                rows = pl.ds(pl.multiple_of(base + step * piece, piece), piece)
                total = sums[0][rows, :]
                for part in sums[1:]:
                    total = total + part[rows, :]
                out[pl.ds(pl.multiple_of(step * piece, piece), piece), :] = total
                return carry

            lax.fori_loop(0, size // piece, add_up, 0)


def scatter_add(place, grads, rows):
    senders = len(grads)
    cap, width = grads[0].shape[0] - 2 * SPARE, grads[0].shape[1]
    chunks = cap // LANES
    shape = jax.ShapeDtypeStruct((rows // (2 * WAVES), width), jnp.float32)
    outs = pl.pallas_call(
        functools.partial(scatter_kernel, senders, cap),
        out_shape=(shape,) * (2 * WAVES),
        in_specs=[SM] + [VM] * senders,
        out_specs=(VM,) * (2 * WAVES),
        scratch_shapes=[pltpu.VMEM((rows + SPARE, width), jnp.float32)] * senders
        + [pltpu.VMEM((cap, width), jnp.float32)] * senders
        + [
            pltpu.VMEM((senders * chunks, LANES), jnp.int32),
            pltpu.SMEM((senders * chunks, LANES), jnp.int32),
            pltpu.SemaphoreType.DMA,
        ],
        compiler_params=room(30),
        cost_estimate=cost(10**8),
        name="scatter",
    )(place, *grads)
    return outs[:WAVES], outs[WAVES:]


def diagonal():
    lane = lax.broadcasted_iota(jnp.int32, (LANES, LANES), 1)
    return lax.broadcasted_iota(jnp.int32, (LANES, LANES), 0) == lane


def to_row(column, diag):
    return jnp.sum(jnp.where(diag, column, 0.0), axis=0, keepdims=True)


def to_column(row, diag):
    return jnp.sum(jnp.where(diag, row, 0.0), axis=1, keepdims=True)


def powers_of(peaks):
    return jnp.ceil(STEPS * jnp.log2(jnp.maximum(peaks, TINY) / TOP))


def short(x):
    return x.astype(jnp.int32).astype(jnp.int16)


def wide_of(x):
    return x.astype(jnp.int32).astype(jnp.float32)


def rounded(x):
    return short((x + ROUNDER) - ROUNDER)


def encode_blocks(block, put, count, peaks, shrinks, diag):
    for k in range(count):
        peak = jnp.max(jnp.abs(block(k)), axis=1, keepdims=True)
        peaks[k : k + 1, :] = to_row(peak, diag)
    powers = powers_of(peaks[...])
    peaks[...] = powers
    shrinks[...] = jnp.exp2(powers * (-1.0 / STEPS))
    for k in range(count):
        tail = short(jnp.broadcast_to(peaks[k : k + 1, :], (SPARE, LANES)))
        put(k, rounded(block(k) * to_column(shrinks[k : k + 1, :], diag)), tail)


def decode(part, diag):
    scale = to_column(jnp.exp2(wide_of(part[LANES:CODED]) * (1.0 / STEPS))[0:1], diag)
    return wide_of(part[0:LANES]) * scale


def encode_kernel(mine, got, out, peaks, shrinks):
    diag = diagonal()
    groups, blocks = out.shape[:2]
    size = blocks * LANES

    def body(group, carry):
        def block(k):
            rows = pl.ds(pl.multiple_of(group * size + k * LANES, LANES), LANES)
            return mine[rows, :] + got[rows, :]

        def put(k, code, tail):
            out[group, k, 0:LANES, :] = code
            out[group, k, LANES:CODED, :] = tail

        encode_blocks(block, put, blocks, peaks, shrinks, diag)
        return carry

    lax.fori_loop(0, groups, body, 0)


def encode_sum(mine, got, groups):
    blocks = mine.shape[0] // (groups * LANES)
    return pl.pallas_call(
        encode_kernel,
        out_shape=jax.ShapeDtypeStruct((groups, blocks, CODED, LANES), jnp.int16),
        in_specs=[VM, VM],
        out_specs=VM,
        scratch_shapes=[pltpu.VMEM((blocks, LANES), jnp.float32)] * 2,
        compiler_params=room(8),
        cost_estimate=cost(10**7),
        name="encode",
    )(mine, got)


def first_sum_kernel(parts, out, totals, peaks, shrinks):
    diag = diagonal()
    groups, blocks = parts.shape[:2]

    def body(k, carry):
        total = decode(parts[0, k], diag)
        for j in range(1, groups):
            total = total + decode(parts[j, k], diag)
        totals[k] = total
        return carry

    lax.fori_loop(0, blocks, body, 0)

    def put(k, code, tail):
        out[k, 0:LANES, :] = code
        out[k, LANES:CODED, :] = tail

    encode_blocks(lambda k: totals[k], put, blocks, peaks, shrinks, diag)


def first_sum(parts):
    blocks = parts.shape[1]
    return pl.pallas_call(
        first_sum_kernel,
        out_shape=jax.ShapeDtypeStruct(parts.shape[1:], jnp.int16),
        in_specs=[VM],
        out_specs=VM,
        scratch_shapes=[pltpu.VMEM((blocks, LANES, LANES), jnp.float32)]
        + [pltpu.VMEM((blocks, LANES), jnp.float32)] * 2,
        compiler_params=room(6),
        cost_estimate=cost(10**7),
        name="first_sum",
    )(parts)


def last_sum_kernel(parts, out):
    diag = diagonal()
    total = decode(parts[0], diag)
    for j in range(1, parts.shape[0]):
        total = total + decode(parts[j], diag)
    powers = powers_of(to_row(jnp.max(jnp.abs(total), axis=1, keepdims=True), diag))
    code = rounded(total * to_column(jnp.exp2(powers * (-1.0 / STEPS)), diag))
    tail = short(jnp.broadcast_to(powers, (SPARE, LANES)))
    for j in range(out.shape[0]):
        out[j, 0:LANES, :] = code
        out[j, LANES:CODED, :] = tail


def last_sum(parts):
    return pl.pallas_call(
        last_sum_kernel,
        out_shape=jax.ShapeDtypeStruct(parts.shape, jnp.int16),
        in_specs=[VM],
        out_specs=VM,
        compiler_params=room(4),
        cost_estimate=cost(10**6),
        name="last_sum",
    )(parts)


def update_kernel(count, groups, core, *refs):
    mine, got = refs[:count], refs[count : 2 * count]
    rows, state = refs[2 * count : 2 * count + 2]
    new_rows, new_state, held, loaded, sems, sums, scales = refs[-7:]
    step = pl.program_id(0)
    tables, blocks = held.shape[:2]
    size = blocks * LANES

    def load(d):
        first = pl.multiple_of(groups[d] * size, size)
        return pltpu.make_async_copy(rows.at[:, pl.ds(first, size), :], loaded.at[d], sems.at[d])

    @pl.when(step == 0)
    def _():
        for d in range(count):
            load(d).start()

    for d in range(count):

        @pl.when(step == d)
        def _():
            held[core[0]] = mine[d][...]
            held[1 - core[0]] = got[d][...]

    diag = diagonal()
    start = groups[step] * size
    every = [(table, k) for table in range(tables) for k in range(blocks)]
    for at, (table, k) in enumerate(every):
        code = wide_of(held[table, k, 0:LANES, :])
        sums[at : at + 1, :] = to_row(jnp.sum(code * code, axis=1, keepdims=True), diag)
        scales[at : at + 1, :] = wide_of(held[table, k, LANES:CODED, :])[0:1]
    scale = jnp.exp2(scales[...] * (1.0 / STEPS))
    gain = sums[...] * (scale * scale) * (1.0 / LANES)
    for at, (table, k) in enumerate(every):
        lanes = slice(k * LANES, (k + 1) * LANES)
        there = pl.ds(pl.multiple_of(start + k * LANES, LANES), LANES)
        updated = state[table : table + 1, there] + gain[at : at + 1, :]
        new_state[table : table + 1, lanes] = updated
        sums[at : at + 1, :] = updated
    scales[...] = LEARN_RATE * scale / (jnp.sqrt(sums[...]) + EPSILON)
    load(step).wait()
    for at, (table, k) in enumerate(every):
        there = slice(k * LANES, (k + 1) * LANES)
        move = wide_of(held[table, k, 0:LANES, :]) * to_column(scales[at : at + 1, :], diag)
        new_rows[table, there, :] = loaded[step, table, there, :] - move


def update(groups, core, mine, got, rows, state, earlier):
    tables, rows_dev, width = rows.shape
    count = len(mine)
    blocks = mine[0].shape[0]
    size = blocks * LANES
    row_spec = pl.BlockSpec((tables, size, width), lambda i, g, c: (0, g[i], 0))
    state_spec = pl.BlockSpec((tables, size), lambda i, g, c: (0, g[i]))
    first = 2 + 2 * count + 2
    anywhere = pl.BlockSpec(memory_space=pl.ANY)
    return pl.pallas_call(
        functools.partial(update_kernel, count),
        grid_spec=pltpu.PrefetchScalarGridSpec(
            num_scalar_prefetch=2,
            grid=(count,),
            in_specs=[VM] * (2 * count) + [anywhere, VM] + [anywhere] * len(earlier),
            out_specs=(row_spec, state_spec),
            scratch_shapes=[
                pltpu.VMEM((tables, *mine[0].shape), jnp.int16),
                pltpu.VMEM((count, tables, size, width), jnp.float32),
                pltpu.SemaphoreType.DMA((count,)),
            ]
            + [pltpu.VMEM((tables * blocks, LANES), jnp.float32)] * 2,
        ),
        out_shape=(
            jax.ShapeDtypeStruct(rows.shape, jnp.float32),
            jax.ShapeDtypeStruct(state.shape, jnp.float32),
        ),
        input_output_aliases={first: 0, first + 1: 1} if earlier else {},
        compiler_params=room(12),
        cost_estimate=cost(10**7),
        name="update",
    )(groups, core, *mine, *got, rows, state, *earlier)


def shift(x, axis, by):
    count = lax.axis_size(axis)
    return lax.ppermute(x, axis, [(i, (i + by) % count) for i in range(count)])


def square_shift(x, pair_by, ring_by):
    pairs, rings = lax.axis_size("pair"), lax.axis_size("ring")
    links = [
        (p * rings + r, (p + pair_by) % pairs * rings + (r + ring_by) % rings)
        for p in range(pairs)
        for r in range(rings)
    ]
    return lax.ppermute(x, SQUARE, links)


def lane_view(slots):
    owners, cap = slots.shape[1:]
    return slots.reshape(owners, cap // LANES, LANES).transpose(1, 0, 2)


def shards(pooled_grad, slot_source, slot_target, slot_count, table_rows, accum):
    feature = pooled_grad.shape[2]
    tables, rows_dev, _ = table_rows.shape
    owners = slot_source.shape[1]
    pairs, rings = lax.axis_size("pair"), lax.axis_size("ring")
    row, core, pair, ring = (lax.axis_index(a) for a in ("rows", "core", "pair", "ring"))
    hops = [(0, 0), (0, 1), (0, 3), (1, 0), (1, 1), (1, 3), (0, 2), (1, 2)]
    behind = [(pair + p) % pairs * rings + (ring + rings - r) % rings for p, r in hops]
    facts = jnp.stack([row, core, *behind]).astype(jnp.int32)
    place, core, behind = facts[0:2], facts[1:2], facts[2:]
    flat_grad = pooled_grad.reshape(-1, feature)
    keys, targets = lane_view(slot_source), lane_view(slot_target)

    grads = [None] * owners
    for group in ((2,), (1, 3), (0,)):
        picked = pick_rows(group, tables * rows_dev, place, slot_count, keys, targets, flat_grad)
        for hop, block in zip(group, picked):
            grads[hop] = shift(block, "rows", hop) if hop else block
    (mine,), (other,) = scatter_add(place, grads, tables * rows_dev)
    coded = encode_sum(mine, shift(other, "core", 1), pairs * rings)
    parts = lax.all_to_all(coded, SQUARE, 0, 0, tiled=True)
    parts = lax.all_to_all(first_sum(parts), "far", 0, 0, tiled=True)
    bundle = lax.all_to_all(last_sum(parts), "far", 0, 0, tiled=True)
    whole = [None] * len(hops)
    for d in reversed(range(len(hops))):
        whole[d] = square_shift(bundle, *hops[d]) if d else bundle
    swapped = [shift(w, "core", 1) for w in whole]
    result = ()
    for part in (slice(0, 4), slice(4, 8)):
        result = update(
            behind[part], core, whole[part], swapped[part], table_rows, accum, result
        )
    return result


def solution(mesh):
    split = Mesh(mesh.devices.reshape(4, 2, 4, 2, mesh.shape["rows"]), AXES)
    placed = (
        P(AXES, None, None),
        P(AXES, None, None),
        P(AXES, None, None),
        P(AXES, None),
        P(None, "rows", None),
        P(None, "rows"),
    )
    return jax.shard_map(
        shards,
        mesh=split,
        in_specs=placed,
        out_specs=(P(None, "rows", None), P(None, "rows")),
        check_vma=False,
    )
```

```python
import functools

import jax
import jax.numpy as jnp
from jax import lax
from jax.experimental import pallas as pl
from jax.experimental.pallas import tpu as pltpu
from jax.sharding import Mesh
from jax.sharding import PartitionSpec as P


AXES = ("far", "pair", "ring", "core", "rows")
SQUARE = ("pair", "ring")

LEARN_RATE = 0.1
EPSILON = 1e-06
LANES = 128
SPARE = 8
CODED = LANES + SPARE
STEPS = 64.0
TOP = 32700.0
TINY = 1e-30
ROUNDER = 12582912.0

VM = pl.BlockSpec(memory_space=pltpu.VMEM)
SM = pl.BlockSpec(memory_space=pltpu.SMEM)
HB = pl.BlockSpec(memory_space=pltpu.HBM)


def room(mib):
    return pltpu.CompilerParams(vmem_limit_bytes=mib * 2**20)


def cost(flops):
    return pl.CostEstimate(flops=flops, bytes_accessed=10**6, transcendentals=0)


def loop(count, body):
    def step(i, carry):
        body(i)
        return carry

    lax.fori_loop(0, count, step, 0)


def pieces(count, size, body):
    loop(count // size, lambda i: body(pl.ds(pl.multiple_of(i * size, size), size)))


def pick(owner, keys, held, wide, out, stage):
    chunks = keys.shape[0]
    cap = chunks * LANES

    def body(chunk):
        first = chunk * LANES
        for u in range(LANES):
            key = keys[chunk, owner, u]
            stage[pl.ds(first + u, 1), :] = wide[pl.ds(key, 1), :]

    loop(chunks, body)

    def narrow(rows):
        out[rows, :] = stage[rows, :].astype(jnp.bfloat16)

    pieces(cap, LANES, narrow)
    target = held[owner]
    upper = target >> 7
    out[cap : cap + SPARE, :] = upper.astype(jnp.float32).astype(jnp.bfloat16)
    lower = target - upper * LANES
    out[cap + SPARE : cap + 2 * SPARE, :] = lower.astype(jnp.float32).astype(jnp.bfloat16)


def first_pick_kernel(
    hop, unused, place, count, keys, keys_in, targets, flat, out, wide, held, kept, stage
):
    chunks, owners, _ = targets.shape
    slots = lax.broadcasted_iota(jnp.int32, (chunks, LANES), 0) * LANES
    slots = slots + lax.broadcasted_iota(jnp.int32, (chunks, LANES), 1)
    kept[...] = keys_in[...]
    for owner in range(owners):
        held[owner] = jnp.where(slots < count[0, owner], targets[:, owner, :], unused)

    def widen(rows):
        wide[rows, :] = flat[rows, :].astype(jnp.float32)

    pieces(flat.shape[0], LANES, widen)
    pick(lax.rem(place[0] + hop, owners), keys, held, wide, out, stage)


def first_pick(hop, unused, place, count, keys, targets, flat):
    chunks, owners, _ = keys.shape
    cap = chunks * LANES
    width = flat.shape[1]
    return pl.pallas_call(
        functools.partial(first_pick_kernel, hop, unused),
        out_shape=(
            jax.ShapeDtypeStruct((cap + 2 * SPARE, width), jnp.bfloat16),
            jax.ShapeDtypeStruct(flat.shape, jnp.float32),
            jax.ShapeDtypeStruct((owners, chunks, LANES), jnp.int32),
            jax.ShapeDtypeStruct(keys.shape, jnp.int32),
        ),
        in_specs=[SM, SM, SM, VM, VM, VM],
        out_specs=(VM, VM, VM, VM),
        scratch_shapes=[pltpu.VMEM((cap, width), jnp.float32)],
        compiler_params=room(6),
        cost_estimate=cost(10**7),
        name="first_pick",
    )(place, count, keys, keys, targets, flat)


def pick_kernel(hops, place, keys, held, wide, *refs):
    outs, stages = refs[: len(hops)], refs[len(hops) :]
    owners = held.shape[0]
    for hop, out, stage in zip(hops, outs, stages):
        pick(lax.rem(place[0] + hop, owners), keys, held, wide, out, stage)


def pick_rows(hops, place, keys, held, wide):
    cap = keys.shape[0] * LANES
    width = wide.shape[1]
    shape = jax.ShapeDtypeStruct((cap + 2 * SPARE, width), jnp.bfloat16)
    return pl.pallas_call(
        functools.partial(pick_kernel, hops),
        out_shape=(shape,) * len(hops),
        in_specs=[SM, SM, VM, VM],
        out_specs=(VM,) * len(hops),
        scratch_shapes=[pltpu.VMEM((cap, width), jnp.float32)] * len(hops),
        compiler_params=room(6),
        cost_estimate=cost(10**7 * len(hops)),
        name="pick",
    )(place, keys, held, wide)


def add_rows(pairs, sums, wides, keys, rows, chunk):
    first = chunk * LANES
    for u in range(0, LANES, 2 * pairs):
        for k, row in enumerate(rows):
            for p in range(pairs):
                at, total = u + 2 * p, sums[k * pairs + p]
                one, two = keys[row + chunk, at], keys[row + chunk, at + 1]
                here, next_ = pl.ds(one, 1), pl.ds(two, 1)
                again = jnp.where(one == two, 1.0, 0.0)
                lead = wides[k][pl.ds(first + at, 1), :]
                tail = wides[k][pl.ds(first + at + 1, 1), :] + lead * again
                before, after = total[here, :], total[next_, :]
                total[here, :] = before + lead
                total[next_, :] = after + tail


def prepare(grads, cap, sums, wides, found, keys, sem):
    chunks = cap // LANES
    for k, grad in enumerate(grads):
        upper = grad[cap : cap + SPARE, :].astype(jnp.float32)
        lower = grad[cap + SPARE : cap + 2 * SPARE, :].astype(jnp.float32)
        found[k * chunks : (k + 1) * chunks, :] = (upper * LANES + lower).astype(jnp.int32)
    copy = pltpu.make_async_copy(found, keys, sem)
    copy.start()

    def widen(rows):
        for wide, grad in zip(wides, grads):
            wide[rows, :] = grad[rows, :].astype(jnp.float32)

    def clear(rows):
        for total in sums:
            total[rows, :] = jnp.zeros((64, LANES), jnp.float32)

    pieces(cap, 64, widen)
    pieces(sums[0].shape[0] // 64 * 64, 64, clear)
    copy.wait()


def own_kernel(parts, place, keys, held, wide, out, *refs):
    sums, (found, sem) = refs[:parts], refs[parts:]
    owner = place[0]
    copy = pltpu.make_async_copy(held.at[owner], found, sem)
    copy.start()

    def clear(rows):
        for total in sums:
            total[rows, :] = jnp.zeros((64, LANES), jnp.float32)

    pieces(sums[0].shape[0] // 64 * 64, 64, clear)
    copy.wait()

    def body(chunk):
        for u in range(0, LANES, 2 * parts):
            for p, total in enumerate(sums):
                at = u + 2 * p
                one, two = found[chunk, at], found[chunk, at + 1]
                lead = wide[pl.ds(keys[chunk, owner, at], 1), :]
                tail = wide[pl.ds(keys[chunk, owner, at + 1], 1), :]
                tail = tail + lead * jnp.where(one == two, 1.0, 0.0)
                here, next_ = pl.ds(one, 1), pl.ds(two, 1)
                before, after = total[here, :], total[next_, :]
                total[here, :] = before + lead
                total[next_, :] = after + tail

    loop(keys.shape[0], body)

    def add_up(rows):
        total = sums[0][rows, :]
        for part in sums[1:]:
            total = total + part[rows, :]
        out[rows, :] = total

    pieces(out.shape[0], 64, add_up)


def scatter_kernel(cap, senders, place, begun, *refs):
    grads, outs, refs = refs[:senders], refs[senders : senders + 2], refs[senders + 2 :]
    sums, wides = refs[:senders], refs[senders : 2 * senders]
    found, keys, sem = refs[2 * senders :]
    chunks = cap // LANES
    prepare(grads, cap, sums, wides, found, keys, sem)
    rows = [k * chunks for k in range(senders)]
    loop(chunks, lambda chunk: add_rows(1, sums, wides, keys, rows, chunk))
    half = outs[0].shape[0]
    for out, index in ((outs[1], 1 - place[1]), (outs[0], place[1])):

        def add_up(i):
            there = pl.ds(pl.multiple_of(index * half + i * 64, 64), 64)
            total = begun[there, :]
            for part in sums:
                total = total + part[there, :]
            out[pl.ds(pl.multiple_of(i * 64, 64), 64), :] = total

        loop(half // 64, add_up)


def tables_of(rows, width, cap, senders, pairs):
    chunks = cap // LANES
    return (
        [pltpu.VMEM((rows + SPARE, width), jnp.float32)] * (senders * pairs)
        + [pltpu.VMEM((cap, width), jnp.float32)] * senders
        + [
            pltpu.VMEM((senders * chunks, LANES), jnp.int32),
            pltpu.SMEM((senders * chunks, LANES), jnp.int32),
            pltpu.SemaphoreType.DMA,
        ]
    )


def own_rows(place, keys, held, wide, rows):
    width = wide.shape[1]
    parts = 2
    return pl.pallas_call(
        functools.partial(own_kernel, parts),
        out_shape=jax.ShapeDtypeStruct((rows, width), jnp.float32),
        in_specs=[SM, SM, VM, VM],
        out_specs=VM,
        scratch_shapes=[pltpu.VMEM((rows + SPARE, width), jnp.float32)] * parts
        + [pltpu.SMEM(held.shape[1:], jnp.int32), pltpu.SemaphoreType.DMA],
        compiler_params=room(16),
        cost_estimate=cost(10**7),
        name="own_rows",
    )(place, keys, held, wide)


def scatter_add(place, begun, grads):
    senders = len(grads)
    cap, width = grads[0].shape[0] - 2 * SPARE, grads[0].shape[1]
    rows = begun.shape[0]
    shape = jax.ShapeDtypeStruct((rows // 2, width), jnp.float32)
    return pl.pallas_call(
        functools.partial(scatter_kernel, cap, senders),
        out_shape=(shape, shape),
        in_specs=[SM, VM] + [VM] * senders,
        out_specs=(VM, VM),
        scratch_shapes=tables_of(rows, width, cap, senders, 1),
        compiler_params=room(24),
        cost_estimate=cost(10**8),
        name="scatter",
    )(place, begun, *grads)


def diagonal():
    lane = lax.broadcasted_iota(jnp.int32, (LANES, LANES), 1)
    return lax.broadcasted_iota(jnp.int32, (LANES, LANES), 0) == lane


def to_row(column, diag):
    return jnp.sum(jnp.where(diag, column, 0.0), axis=0, keepdims=True)


def to_column(row, diag):
    return jnp.sum(jnp.where(diag, row, 0.0), axis=1, keepdims=True)


def powers_of(peaks):
    return jnp.ceil(STEPS * jnp.log2(jnp.maximum(peaks, TINY) / TOP))


def short(x):
    return x.astype(jnp.int32).astype(jnp.int16)


def wide_of(x):
    return x.astype(jnp.int32).astype(jnp.float32)


def rounded(x):
    return short((x + ROUNDER) - ROUNDER)


def encode_blocks(block, put, count, peaks, shrinks, diag):
    for k in range(count):
        peak = jnp.max(jnp.abs(block(k)), axis=1, keepdims=True)
        peaks[k : k + 1, :] = to_row(peak, diag)
    powers = powers_of(peaks[...])
    peaks[...] = powers
    shrinks[...] = jnp.exp2(powers * (-1.0 / STEPS))
    for k in range(count):
        tail = short(jnp.broadcast_to(peaks[k : k + 1, :], (SPARE, LANES)))
        put(k, rounded(block(k) * to_column(shrinks[k : k + 1, :], diag)), tail)


def decode(part, diag):
    scale = to_column(jnp.exp2(wide_of(part[LANES:CODED]) * (1.0 / STEPS))[0:1], diag)
    return wide_of(part[0:LANES]) * scale


def encode_kernel(mine, got, out, peaks, shrinks):
    diag = diagonal()
    groups, blocks = out.shape[:2]
    size = blocks * LANES

    def body(group, carry):
        def block(k):
            rows = pl.ds(pl.multiple_of(group * size + k * LANES, LANES), LANES)
            return mine[rows, :] + got[rows, :]

        def put(k, code, tail):
            out[group, k, 0:LANES, :] = code
            out[group, k, LANES:CODED, :] = tail

        encode_blocks(block, put, blocks, peaks, shrinks, diag)
        return carry

    lax.fori_loop(0, groups, body, 0)


def encode_sum(mine, got, groups):
    blocks = mine.shape[0] // (groups * LANES)
    return pl.pallas_call(
        encode_kernel,
        out_shape=jax.ShapeDtypeStruct((groups, blocks, CODED, LANES), jnp.int16),
        in_specs=[VM, VM],
        out_specs=VM,
        scratch_shapes=[pltpu.VMEM((blocks, LANES), jnp.float32)] * 2,
        compiler_params=room(8),
        cost_estimate=cost(10**7),
        name="encode",
    )(mine, got)


def first_sum_kernel(parts, out, totals, peaks, shrinks):
    diag = diagonal()
    groups, blocks = parts.shape[:2]

    def body(k, carry):
        total = decode(parts[0, k], diag)
        for j in range(1, groups):
            total = total + decode(parts[j, k], diag)
        totals[k] = total
        return carry

    lax.fori_loop(0, blocks, body, 0)

    def put(k, code, tail):
        out[k, 0:LANES, :] = code
        out[k, LANES:CODED, :] = tail

    encode_blocks(lambda k: totals[k], put, blocks, peaks, shrinks, diag)


def first_sum(parts):
    blocks = parts.shape[1]
    return pl.pallas_call(
        first_sum_kernel,
        out_shape=jax.ShapeDtypeStruct(parts.shape[1:], jnp.int16),
        in_specs=[VM],
        out_specs=VM,
        scratch_shapes=[pltpu.VMEM((blocks, LANES, LANES), jnp.float32)]
        + [pltpu.VMEM((blocks, LANES), jnp.float32)] * 2,
        compiler_params=room(6),
        cost_estimate=cost(10**7),
        name="first_sum",
    )(parts)


def last_sum_kernel(parts, out):
    diag = diagonal()
    total = decode(parts[0], diag)
    for j in range(1, parts.shape[0]):
        total = total + decode(parts[j], diag)
    powers = powers_of(to_row(jnp.max(jnp.abs(total), axis=1, keepdims=True), diag))
    code = rounded(total * to_column(jnp.exp2(powers * (-1.0 / STEPS)), diag))
    tail = short(jnp.broadcast_to(powers, (SPARE, LANES)))
    for j in range(out.shape[0]):
        out[j, 0:LANES, :] = code
        out[j, LANES:CODED, :] = tail


def last_sum(parts):
    return pl.pallas_call(
        last_sum_kernel,
        out_shape=jax.ShapeDtypeStruct(parts.shape, jnp.int16),
        in_specs=[VM],
        out_specs=VM,
        compiler_params=room(4),
        cost_estimate=cost(10**6),
        name="last_sum",
    )(parts)


def update_kernel(count, groups, core, *refs):
    mine, got = refs[:count], refs[count : 2 * count]
    rows, state = refs[2 * count : 2 * count + 2]
    new_rows, new_state, held, sums, scales = refs[-5:]
    step = pl.program_id(0)
    tables, blocks = held.shape[:2]
    size = blocks * LANES
    for d in range(count):

        @pl.when(step == d)
        def _():
            held[core[0]] = mine[d][...]
            held[1 - core[0]] = got[d][...]

    diag = diagonal()
    start = groups[step] * size
    every = [(table, k) for table in range(tables) for k in range(blocks)]
    for at, (table, k) in enumerate(every):
        code = wide_of(held[table, k, 0:LANES, :])
        sums[at : at + 1, :] = to_row(jnp.sum(code * code, axis=1, keepdims=True), diag)
        scales[at : at + 1, :] = wide_of(held[table, k, LANES:CODED, :])[0:1]
    scale = jnp.exp2(scales[...] * (1.0 / STEPS))
    gain = sums[...] * (scale * scale) * (1.0 / LANES)
    for at, (table, k) in enumerate(every):
        lanes = slice(k * LANES, (k + 1) * LANES)
        there = pl.ds(pl.multiple_of(start + k * LANES, LANES), LANES)
        updated = state[table : table + 1, there] + gain[at : at + 1, :]
        new_state[table : table + 1, lanes] = updated
        sums[at : at + 1, :] = updated
    scales[...] = LEARN_RATE * scale / (jnp.sqrt(sums[...]) + EPSILON)
    for at, (table, k) in enumerate(every):
        there = slice(k * LANES, (k + 1) * LANES)
        move = wide_of(held[table, k, 0:LANES, :]) * to_column(scales[at : at + 1, :], diag)
        new_rows[table, there, :] = rows[step, table, there, :] - move


def update(groups, core, mine, got, rows, state, earlier):
    count, tables, size, width = rows.shape
    blocks = mine[0].shape[0]
    row_spec = pl.BlockSpec((tables, size, width), lambda i, g, c: (0, g[i], 0))
    state_spec = pl.BlockSpec((tables, size), lambda i, g, c: (0, g[i]))
    first = 2 + 2 * count + 2
    return pl.pallas_call(
        functools.partial(update_kernel, count),
        grid_spec=pltpu.PrefetchScalarGridSpec(
            num_scalar_prefetch=2,
            grid=(count,),
            in_specs=[VM] * (2 * count) + [VM, VM] + [HB] * len(earlier),
            out_specs=(row_spec, state_spec),
            scratch_shapes=[
                pltpu.VMEM((tables, *mine[0].shape), jnp.int16),
            ]
            + [pltpu.VMEM((tables * blocks, LANES), jnp.float32)] * 2,
        ),
        out_shape=(
            jax.ShapeDtypeStruct((tables, state.shape[1], width), jnp.float32),
            jax.ShapeDtypeStruct(state.shape, jnp.float32),
        ),
        input_output_aliases={first: 0, first + 1: 1} if earlier else {},
        compiler_params=room(12),
        cost_estimate=cost(10**7),
        name="update",
    )(groups, core, *mine, *got, rows, state, *earlier)


def fetch_kernel(groups, rows, after, *refs):
    outs, sems = refs[:-1], refs[-1]
    count, _, size, _ = outs[0].shape
    copies = []
    for i, out in enumerate(outs):
        for d in range(count):
            at = i * count + d
            there = pl.ds(pl.multiple_of(groups[at] * size, size), size)
            copies.append(pltpu.make_async_copy(rows.at[:, there, :], out.at[d], sems.at[at]))
    for copy in copies:
        copy.start()
    for copy in copies:
        copy.wait()


def fetch(groups, rows, after):
    tables, rows_dev, width = rows.shape
    count = groups.shape[0]
    shape = jax.ShapeDtypeStruct((count // 2, tables, rows_dev // count, width), rows.dtype)
    return pl.pallas_call(
        fetch_kernel,
        out_shape=(shape, shape),
        in_specs=[SM, HB, HB],
        out_specs=(VM, VM),
        scratch_shapes=[pltpu.SemaphoreType.DMA((count,))],
        compiler_params=room(5),
        cost_estimate=cost(3 * 10**7),
        name="fetch",
    )(groups, rows, after)


def shift(x, axis, by):
    count = lax.axis_size(axis)
    return lax.ppermute(x, axis, [(i, (i + by) % count) for i in range(count)])


def square_shift(x, pair_by, ring_by):
    pairs, rings = lax.axis_size("pair"), lax.axis_size("ring")
    links = [
        (p * rings + r, (p + pair_by) % pairs * rings + (r + ring_by) % rings)
        for p in range(pairs)
        for r in range(rings)
    ]
    return lax.ppermute(x, SQUARE, links)


def lane_view(slots):
    owners, cap = slots.shape[1:]
    return slots.reshape(owners, cap // LANES, LANES).transpose(1, 0, 2)


def shards(pooled_grad, slot_source, slot_target, slot_count, table_rows, accum):
    feature = pooled_grad.shape[2]
    tables, rows_dev, _ = table_rows.shape
    pairs, rings = lax.axis_size("pair"), lax.axis_size("ring")
    row, core, pair, ring = (lax.axis_index(a) for a in ("rows", "core", "pair", "ring"))
    hops = [(0, 0), (0, 1), (0, 3), (1, 0), (1, 1), (1, 3), (0, 2), (1, 2)]
    behind = [(pair + p) % pairs * rings + (ring + rings - r) % rings for p, r in hops]
    facts = jnp.stack([row, core, *behind]).astype(jnp.int32)
    place, core, behind = facts[0:2], facts[1:2], facts[2:]
    flat_grad = pooled_grad.reshape(-1, feature)
    keys, targets = lane_view(slot_source), lane_view(slot_target)

    rows = tables * rows_dev
    first, wide, held, keys = first_pick(2, rows, place, slot_count, keys, targets, flat_grad)
    picked = {2: first}
    picked.update(zip((1, 3), pick_rows((1, 3), place, keys, held, wide)))
    grads = []
    for hop, block in picked.items():
        grads.append(shift(block, "rows", hop))
    begun = own_rows(place, keys, held, wide, rows)
    mine, other = scatter_add(place, begun, grads)
    order = ((7, 6, 5, 0), (4, 3, 2, 1))
    behind = jnp.stack([behind[d] for part in order for d in part])
    fetched = fetch(behind, table_rows, begun)
    got = shift(other, "core", 1)
    coded = encode_sum(mine, got, pairs * rings)
    parts = lax.all_to_all(coded, SQUARE, 0, 0, tiled=True)
    parts = lax.all_to_all(first_sum(parts), "far", 0, 0, tiled=True)
    bundle = lax.all_to_all(last_sum(parts), "far", 0, 0, tiled=True)
    whole = [None] * len(hops)
    for d in reversed(range(len(hops))):
        whole[d] = square_shift(bundle, *hops[d]) if d else bundle
    swapped = [shift(w, "core", 1) for w in whole]
    result = ()
    for i in range(2):
        result = update(
            behind[4 * i : 4 * i + 4],
            core,
            [whole[d] for d in order[i]],
            [swapped[d] for d in order[i]],
            fetched[i],
            accum,
            result,
        )
    return result


def solution(mesh):
    split = Mesh(mesh.devices.reshape(4, 2, 4, 2, mesh.shape["rows"]), AXES)
    placed = (
        P(AXES, None, None),
        P(AXES, None, None),
        P(AXES, None, None),
        P(AXES, None),
        P(None, "rows", None),
        P(None, "rows"),
    )

    return jax.shard_map(
        shards,
        mesh=split,
        in_specs=placed,
        out_specs=(P(None, "rows", None), P(None, "rows")),
        check_vma=False,
    )
```

```python
import functools

import jax
import jax.numpy as jnp
from jax import lax
from jax.experimental import pallas as pl
from jax.experimental.pallas import tpu as pltpu
from jax.sharding import Mesh
from jax.sharding import PartitionSpec as P


AXES = ("far", "pair", "ring", "core", "rows")
SQUARE = ("pair", "ring")

LEARN_RATE = 0.1
EPSILON = 1e-06
LANES = 128
SPARE = 8
CODED = LANES + SPARE
STEPS = 64.0
TOP = 32700.0
TINY = 1e-30
ROUNDER = 12582912.0

VM = pl.BlockSpec(memory_space=pltpu.VMEM)
SM = pl.BlockSpec(memory_space=pltpu.SMEM)
HB = pl.BlockSpec(memory_space=pltpu.HBM)


def room(mib):
    return pltpu.CompilerParams(vmem_limit_bytes=mib * 2**20)


def cost(flops):
    return pl.CostEstimate(flops=flops, bytes_accessed=10**6, transcendentals=0)


def loop(count, body):
    def step(i, carry):
        body(i)
        return carry

    lax.fori_loop(0, count, step, 0)


def pieces(count, size, body):
    loop(count // size, lambda i: body(pl.ds(pl.multiple_of(i * size, size), size)))


def pick(owner, keys, held, wide, out, stage):
    chunks = keys.shape[0]
    cap = chunks * LANES

    def body(chunk):
        first = chunk * LANES
        for u in range(LANES):
            key = keys[chunk, owner, u]
            stage[pl.ds(first + u, 1), :] = wide[pl.ds(key, 1), :]

    loop(chunks, body)

    def narrow(rows):
        out[rows, :] = stage[rows, :].astype(jnp.bfloat16)

    pieces(cap, LANES, narrow)
    target = held[owner]
    upper = target >> 7
    out[cap : cap + SPARE, :] = upper.astype(jnp.float32).astype(jnp.bfloat16)
    lower = target - upper * LANES
    out[cap + SPARE : cap + 2 * SPARE, :] = lower.astype(jnp.float32).astype(jnp.bfloat16)


def first_pick_kernel(
    hop, unused, place, count, keys, keys_in, targets, flat, out, wide, held, kept, stage
):
    chunks, owners, _ = targets.shape
    slots = lax.broadcasted_iota(jnp.int32, (chunks, LANES), 0) * LANES
    slots = slots + lax.broadcasted_iota(jnp.int32, (chunks, LANES), 1)
    kept[...] = keys_in[...]
    for owner in range(owners):
        held[owner] = jnp.where(slots < count[0, owner], targets[:, owner, :], unused)

    def widen(rows):
        wide[rows, :] = flat[rows, :].astype(jnp.float32)

    pieces(flat.shape[0], LANES, widen)
    pick(lax.rem(place[0] + hop, owners), keys, held, wide, out, stage)


def first_pick(hop, unused, place, count, keys, targets, flat):
    chunks, owners, _ = keys.shape
    cap = chunks * LANES
    width = flat.shape[1]
    return pl.pallas_call(
        functools.partial(first_pick_kernel, hop, unused),
        out_shape=(
            jax.ShapeDtypeStruct((cap + 2 * SPARE, width), jnp.bfloat16),
            jax.ShapeDtypeStruct(flat.shape, jnp.float32),
            jax.ShapeDtypeStruct((owners, chunks, LANES), jnp.int32),
            jax.ShapeDtypeStruct(keys.shape, jnp.int32),
        ),
        in_specs=[SM, SM, SM, VM, VM, VM],
        out_specs=(VM, VM, VM, VM),
        scratch_shapes=[pltpu.VMEM((cap, width), jnp.float32)],
        compiler_params=room(6),
        cost_estimate=cost(10**7),
        name="first_pick",
    )(place, count, keys, keys, targets, flat)


def pick_kernel(hops, place, keys, held, wide, *refs):
    outs, stages = refs[: len(hops)], refs[len(hops) :]
    owners = held.shape[0]
    for hop, out, stage in zip(hops, outs, stages):
        pick(lax.rem(place[0] + hop, owners), keys, held, wide, out, stage)


def pick_rows(hops, place, keys, held, wide):
    cap = keys.shape[0] * LANES
    width = wide.shape[1]
    shape = jax.ShapeDtypeStruct((cap + 2 * SPARE, width), jnp.bfloat16)
    return pl.pallas_call(
        functools.partial(pick_kernel, hops),
        out_shape=(shape,) * len(hops),
        in_specs=[SM, SM, VM, VM],
        out_specs=(VM,) * len(hops),
        scratch_shapes=[pltpu.VMEM((cap, width), jnp.float32)] * len(hops),
        compiler_params=room(6),
        cost_estimate=cost(10**7 * len(hops)),
        name="pick",
    )(place, keys, held, wide)


def add_rows(pairs, sums, wides, keys, rows, chunk):
    first = chunk * LANES
    for u in range(0, LANES, 2 * pairs):
        for k, row in enumerate(rows):
            for p in range(pairs):
                at, total = u + 2 * p, sums[k * pairs + p]
                one, two = keys[row + chunk, at], keys[row + chunk, at + 1]
                here, next_ = pl.ds(one, 1), pl.ds(two, 1)
                again = jnp.where(one == two, 1.0, 0.0)
                lead = wides[k][pl.ds(first + at, 1), :]
                tail = wides[k][pl.ds(first + at + 1, 1), :] + lead * again
                before, after = total[here, :], total[next_, :]
                total[here, :] = before + lead
                total[next_, :] = after + tail


def prepare(grads, cap, sums, wides, found, keys, sem):
    chunks = cap // LANES
    for k, grad in enumerate(grads):
        upper = grad[cap : cap + SPARE, :].astype(jnp.float32)
        lower = grad[cap + SPARE : cap + 2 * SPARE, :].astype(jnp.float32)
        found[k * chunks : (k + 1) * chunks, :] = (upper * LANES + lower).astype(jnp.int32)
    copy = pltpu.make_async_copy(found, keys, sem)
    copy.start()

    def widen(rows):
        for wide, grad in zip(wides, grads):
            wide[rows, :] = grad[rows, :].astype(jnp.float32)

    def clear(rows):
        for total in sums:
            total[rows, :] = jnp.zeros((64, LANES), jnp.float32)

    pieces(cap, 64, widen)
    pieces(sums[0].shape[0] // 64 * 64, 64, clear)
    copy.wait()


def own_kernel(parts, place, keys, held, wide, out, *refs):
    sums, (found, sem) = refs[:parts], refs[parts:]
    owner = place[0]
    copy = pltpu.make_async_copy(held.at[owner], found, sem)
    copy.start()

    def clear(rows):
        for total in sums:
            total[rows, :] = jnp.zeros((64, LANES), jnp.float32)

    pieces(sums[0].shape[0] // 64 * 64, 64, clear)
    copy.wait()

    def body(chunk):
        for u in range(0, LANES, 2 * parts):
            for p, total in enumerate(sums):
                at = u + 2 * p
                one, two = found[chunk, at], found[chunk, at + 1]
                lead = wide[pl.ds(keys[chunk, owner, at], 1), :]
                tail = wide[pl.ds(keys[chunk, owner, at + 1], 1), :]
                tail = tail + lead * jnp.where(one == two, 1.0, 0.0)
                here, next_ = pl.ds(one, 1), pl.ds(two, 1)
                before, after = total[here, :], total[next_, :]
                total[here, :] = before + lead
                total[next_, :] = after + tail

    loop(keys.shape[0], body)

    def add_up(rows):
        total = sums[0][rows, :]
        for part in sums[1:]:
            total = total + part[rows, :]
        out[rows, :] = total

    pieces(out.shape[0], 64, add_up)


def scatter_kernel(cap, senders, place, begun, *refs):
    grads, outs, refs = refs[:senders], refs[senders : senders + 2], refs[senders + 2 :]
    sums, wides = refs[:senders], refs[senders : 2 * senders]
    found, keys, sem = refs[2 * senders :]
    chunks = cap // LANES
    prepare(grads, cap, sums, wides, found, keys, sem)
    rows = [k * chunks for k in range(senders)]
    loop(chunks, lambda chunk: add_rows(1, sums, wides, keys, rows, chunk))
    half = outs[0].shape[0]
    for out, index in ((outs[1], 1 - place[1]), (outs[0], place[1])):

        def add_up(i):
            there = pl.ds(pl.multiple_of(index * half + i * 64, 64), 64)
            total = begun[there, :]
            for part in sums:
                total = total + part[there, :]
            out[pl.ds(pl.multiple_of(i * 64, 64), 64), :] = total

        loop(half // 64, add_up)


def tables_of(rows, width, cap, senders, pairs):
    chunks = cap // LANES
    return (
        [pltpu.VMEM((rows + SPARE, width), jnp.float32)] * (senders * pairs)
        + [pltpu.VMEM((cap, width), jnp.float32)] * senders
        + [
            pltpu.VMEM((senders * chunks, LANES), jnp.int32),
            pltpu.SMEM((senders * chunks, LANES), jnp.int32),
            pltpu.SemaphoreType.DMA,
        ]
    )


def own_rows(place, keys, held, wide, rows):
    width = wide.shape[1]
    parts = 2
    return pl.pallas_call(
        functools.partial(own_kernel, parts),
        out_shape=jax.ShapeDtypeStruct((rows, width), jnp.float32),
        in_specs=[SM, SM, VM, VM],
        out_specs=VM,
        scratch_shapes=[pltpu.VMEM((rows + SPARE, width), jnp.float32)] * parts
        + [pltpu.SMEM(held.shape[1:], jnp.int32), pltpu.SemaphoreType.DMA],
        compiler_params=room(16),
        cost_estimate=cost(10**7),
        name="own_rows",
    )(place, keys, held, wide)


def scatter_add(place, begun, grads):
    senders = len(grads)
    cap, width = grads[0].shape[0] - 2 * SPARE, grads[0].shape[1]
    rows = begun.shape[0]
    shape = jax.ShapeDtypeStruct((rows // 2, width), jnp.float32)
    return pl.pallas_call(
        functools.partial(scatter_kernel, cap, senders),
        out_shape=(shape, shape),
        in_specs=[SM, VM] + [VM] * senders,
        out_specs=(VM, VM),
        scratch_shapes=tables_of(rows, width, cap, senders, 1),
        compiler_params=room(24),
        cost_estimate=cost(10**8),
        name="scatter",
    )(place, begun, *grads)


def diagonal():
    lane = lax.broadcasted_iota(jnp.int32, (LANES, LANES), 1)
    return lax.broadcasted_iota(jnp.int32, (LANES, LANES), 0) == lane


def to_row(column, diag):
    return jnp.sum(jnp.where(diag, column, 0.0), axis=0, keepdims=True)


def to_column(row, diag):
    return jnp.sum(jnp.where(diag, row, 0.0), axis=1, keepdims=True)


def powers_of(peaks):
    return jnp.ceil(STEPS * jnp.log2(jnp.maximum(peaks, TINY) / TOP))


def short(x):
    return x.astype(jnp.int32).astype(jnp.int16)


def wide_of(x):
    return x.astype(jnp.int32).astype(jnp.float32)


def rounded(x):
    return short((x + ROUNDER) - ROUNDER)


def encode_blocks(block, put, count, peaks, shrinks, diag):
    for k in range(count):
        peak = jnp.max(jnp.abs(block(k)), axis=1, keepdims=True)
        peaks[k : k + 1, :] = to_row(peak, diag)
    powers = powers_of(peaks[...])
    peaks[...] = powers
    shrinks[...] = jnp.exp2(powers * (-1.0 / STEPS))
    for k in range(count):
        tail = short(jnp.broadcast_to(peaks[k : k + 1, :], (SPARE, LANES)))
        put(k, rounded(block(k) * to_column(shrinks[k : k + 1, :], diag)), tail)


def decode(part, diag):
    scale = to_column(jnp.exp2(wide_of(part[LANES:CODED]) * (1.0 / STEPS))[0:1], diag)
    return wide_of(part[0:LANES]) * scale


def encode_kernel(mine, got, out, peaks, shrinks):
    diag = diagonal()
    groups, blocks = out.shape[:2]
    size = blocks * LANES

    def body(group, carry):
        def block(k):
            rows = pl.ds(pl.multiple_of(group * size + k * LANES, LANES), LANES)
            return mine[rows, :] + got[rows, :]

        def put(k, code, tail):
            out[group, k, 0:LANES, :] = code
            out[group, k, LANES:CODED, :] = tail

        encode_blocks(block, put, blocks, peaks, shrinks, diag)
        return carry

    lax.fori_loop(0, groups, body, 0)


def encode_sum(mine, got, groups):
    blocks = mine.shape[0] // (groups * LANES)
    return pl.pallas_call(
        encode_kernel,
        out_shape=jax.ShapeDtypeStruct((groups, blocks, CODED, LANES), jnp.int16),
        in_specs=[VM, VM],
        out_specs=VM,
        scratch_shapes=[pltpu.VMEM((blocks, LANES), jnp.float32)] * 2,
        compiler_params=room(8),
        cost_estimate=cost(10**7),
        name="encode",
    )(mine, got)


def first_sum_kernel(parts, out, totals, peaks, shrinks):
    diag = diagonal()
    groups, blocks = parts.shape[:2]

    def body(k, carry):
        total = decode(parts[0, k], diag)
        for j in range(1, groups):
            total = total + decode(parts[j, k], diag)
        totals[k] = total
        return carry

    lax.fori_loop(0, blocks, body, 0)

    def put(k, code, tail):
        out[k, 0:LANES, :] = code
        out[k, LANES:CODED, :] = tail

    encode_blocks(lambda k: totals[k], put, blocks, peaks, shrinks, diag)


def first_sum(parts):
    blocks = parts.shape[1]
    return pl.pallas_call(
        first_sum_kernel,
        out_shape=jax.ShapeDtypeStruct(parts.shape[1:], jnp.int16),
        in_specs=[VM],
        out_specs=VM,
        scratch_shapes=[pltpu.VMEM((blocks, LANES, LANES), jnp.float32)]
        + [pltpu.VMEM((blocks, LANES), jnp.float32)] * 2,
        compiler_params=room(6),
        cost_estimate=cost(10**7),
        name="first_sum",
    )(parts)


def last_sum_kernel(parts, out):
    diag = diagonal()
    total = decode(parts[0], diag)
    for j in range(1, parts.shape[0]):
        total = total + decode(parts[j], diag)
    powers = powers_of(to_row(jnp.max(jnp.abs(total), axis=1, keepdims=True), diag))
    code = rounded(total * to_column(jnp.exp2(powers * (-1.0 / STEPS)), diag))
    tail = short(jnp.broadcast_to(powers, (SPARE, LANES)))
    for j in range(out.shape[0]):
        out[j, 0:LANES, :] = code
        out[j, LANES:CODED, :] = tail


def last_sum(parts):
    return pl.pallas_call(
        last_sum_kernel,
        out_shape=jax.ShapeDtypeStruct(parts.shape, jnp.int16),
        in_specs=[VM],
        out_specs=VM,
        compiler_params=room(4),
        cost_estimate=cost(10**6),
        name="last_sum",
    )(parts)


def update_kernel(count, groups, core, *refs):
    mine, got = refs[:count], refs[count : 2 * count]
    rows, state = refs[2 * count : 2 * count + 2]
    new_rows, new_state, held, sums, scales = refs[-5:]
    step = pl.program_id(0)
    tables, blocks = held.shape[:2]
    size = blocks * LANES
    for d in range(count):

        @pl.when(step == d)
        def _():
            held[core[0]] = mine[d][...]
            held[1 - core[0]] = got[d][...]

    diag = diagonal()
    start = groups[step] * size
    every = [(table, k) for table in range(tables) for k in range(blocks)]
    for at, (table, k) in enumerate(every):
        code = wide_of(held[table, k, 0:LANES, :])
        sums[at : at + 1, :] = to_row(jnp.sum(code * code, axis=1, keepdims=True), diag)
        scales[at : at + 1, :] = wide_of(held[table, k, LANES:CODED, :])[0:1]
    scale = jnp.exp2(scales[...] * (1.0 / STEPS))
    gain = sums[...] * (scale * scale) * (1.0 / LANES)
    for at, (table, k) in enumerate(every):
        lanes = slice(k * LANES, (k + 1) * LANES)
        there = pl.ds(pl.multiple_of(start + k * LANES, LANES), LANES)
        updated = state[table : table + 1, there] + gain[at : at + 1, :]
        new_state[table : table + 1, lanes] = updated
        sums[at : at + 1, :] = updated
    scales[...] = LEARN_RATE * scale / (jnp.sqrt(sums[...]) + EPSILON)
    for at, (table, k) in enumerate(every):
        there = slice(k * LANES, (k + 1) * LANES)
        move = wide_of(held[table, k, 0:LANES, :]) * to_column(scales[at : at + 1, :], diag)
        new_rows[table, there, :] = rows[step, table, there, :] - move


def update(groups, core, mine, got, rows, state, earlier):
    count, tables, size, width = rows.shape
    blocks = mine[0].shape[0]
    row_spec = pl.BlockSpec((tables, size, width), lambda i, g, c: (0, g[i], 0))
    state_spec = pl.BlockSpec((tables, size), lambda i, g, c: (0, g[i]))
    first = 2 + 2 * count + 2
    return pl.pallas_call(
        functools.partial(update_kernel, count),
        grid_spec=pltpu.PrefetchScalarGridSpec(
            num_scalar_prefetch=2,
            grid=(count,),
            in_specs=[VM] * (2 * count) + [VM, VM] + [HB] * len(earlier),
            out_specs=(row_spec, state_spec),
            scratch_shapes=[
                pltpu.VMEM((tables, *mine[0].shape), jnp.int16),
            ]
            + [pltpu.VMEM((tables * blocks, LANES), jnp.float32)] * 2,
        ),
        out_shape=(
            jax.ShapeDtypeStruct((tables, state.shape[1], width), jnp.float32),
            jax.ShapeDtypeStruct(state.shape, jnp.float32),
        ),
        input_output_aliases={first: 0, first + 1: 1} if earlier else {},
        compiler_params=room(12),
        cost_estimate=cost(10**7),
        name="update",
    )(groups, core, *mine, *got, rows, state, *earlier)


def fetch_kernel(groups, rows, after, *refs):
    outs, sems = refs[:-1], refs[-1]
    count, _, size, _ = outs[0].shape
    copies = []
    for i, out in enumerate(outs):
        for d in range(count):
            at = i * count + d
            there = pl.ds(pl.multiple_of(groups[at] * size, size), size)
            copies.append(pltpu.make_async_copy(rows.at[:, there, :], out.at[d], sems.at[at]))
    for copy in copies:
        copy.start()
    for copy in copies:
        copy.wait()


def fetch(groups, rows, after):
    tables, rows_dev, width = rows.shape
    count = groups.shape[0]
    shape = jax.ShapeDtypeStruct((count // 2, tables, rows_dev // count, width), rows.dtype)
    return pl.pallas_call(
        fetch_kernel,
        out_shape=(shape, shape),
        in_specs=[SM, HB, HB],
        out_specs=(VM, VM),
        scratch_shapes=[pltpu.SemaphoreType.DMA((count,))],
        compiler_params=room(5),
        cost_estimate=cost(3 * 10**7),
        name="fetch",
    )(groups, rows, after)


def keep_kernel(state, out):
    out[...] = state[...]


def keep(state):
    return pl.pallas_call(
        keep_kernel,
        out_shape=jax.ShapeDtypeStruct(state.shape, state.dtype),
        in_specs=[VM],
        out_specs=VM,
        compiler_params=room(1),
        cost_estimate=cost(10**5),
        name="keep",
    )(state)


def shift(x, axis, by):
    count = lax.axis_size(axis)
    return lax.ppermute(x, axis, [(i, (i + by) % count) for i in range(count)])


def square_shift(x, pair_by, ring_by):
    pairs, rings = lax.axis_size("pair"), lax.axis_size("ring")
    links = [
        (p * rings + r, (p + pair_by) % pairs * rings + (r + ring_by) % rings)
        for p in range(pairs)
        for r in range(rings)
    ]
    return lax.ppermute(x, SQUARE, links)


def lane_view(slots):
    owners, cap = slots.shape[1:]
    return slots.reshape(owners, cap // LANES, LANES).transpose(1, 0, 2)


def shards(pooled_grad, slot_source, slot_target, slot_count, table_rows, accum):
    feature = pooled_grad.shape[2]
    tables, rows_dev, _ = table_rows.shape
    pairs, rings = lax.axis_size("pair"), lax.axis_size("ring")
    row, core, pair, ring = (lax.axis_index(a) for a in ("rows", "core", "pair", "ring"))
    hops = [(0, 0), (0, 1), (0, 3), (1, 0), (1, 1), (1, 3), (0, 2), (1, 2)]
    behind = [(pair + p) % pairs * rings + (ring + rings - r) % rings for p, r in hops]
    facts = jnp.stack([row, core, *behind]).astype(jnp.int32)
    place, core, behind = facts[0:2], facts[1:2], facts[2:]
    flat_grad = pooled_grad.reshape(-1, feature)
    keys, targets = lane_view(slot_source), lane_view(slot_target)

    rows = tables * rows_dev
    first, wide, held, keys = first_pick(2, rows, place, slot_count, keys, targets, flat_grad)
    picked = {2: first}
    picked.update(zip((1, 3), pick_rows((1, 3), place, keys, held, wide)))
    grads = []
    for hop, block in picked.items():
        grads.append(shift(block, "rows", hop))
    begun = own_rows(place, keys, held, wide, rows)
    mine, other = scatter_add(place, begun, grads)
    order = ((7, 6, 5, 0), (4, 3, 2, 1))
    behind = jnp.stack([behind[d] for part in order for d in part])
    fetched = fetch(behind, table_rows, begun)
    got = shift(other, "core", 1)
    coded = encode_sum(mine, got, pairs * rings)
    parts = lax.all_to_all(coded, SQUARE, 0, 0, tiled=True)
    parts = lax.all_to_all(first_sum(parts), "far", 0, 0, tiled=True)
    bundle = lax.all_to_all(last_sum(parts), "far", 0, 0, tiled=True)
    whole = [None] * len(hops)
    for d in reversed(range(len(hops))):
        whole[d] = square_shift(bundle, *hops[d]) if d else bundle
    state = keep(accum)
    swapped = [shift(w, "core", 1) for w in whole]
    result = ()
    for i in range(2):
        result = update(
            behind[4 * i : 4 * i + 4],
            core,
            [whole[d] for d in order[i]],
            [swapped[d] for d in order[i]],
            fetched[i],
            state,
            result,
        )
    return result


def solution(mesh):
    split = Mesh(mesh.devices.reshape(4, 2, 4, 2, mesh.shape["rows"]), AXES)
    placed = (
        P(AXES, None, None),
        P(AXES, None, None),
        P(AXES, None, None),
        P(AXES, None),
        P(None, "rows", None),
        P(None, "rows"),
    )

    return jax.shard_map(
        shards,
        mesh=split,
        in_specs=placed,
        out_specs=(P(None, "rows", None), P(None, "rows")),
        check_vma=False,
    )
```

```python
import functools

import jax
import jax.numpy as jnp
from jax import lax
from jax.experimental import pallas as pl
from jax.experimental.pallas import tpu as pltpu
from jax.sharding import Mesh
from jax.sharding import PartitionSpec as P


AXES = ("far", "pair", "ring", "core", "rows")
SQUARE = ("pair", "ring")

LEARN_RATE = 0.1
EPSILON = 1e-06
LANES = 128
SPARE = 8
CODED = LANES + SPARE
STEPS = 64.0
TOP = 32700.0
TINY = 1e-30
ROUNDER = 12582912.0

VM = pl.BlockSpec(memory_space=pltpu.VMEM)
SM = pl.BlockSpec(memory_space=pltpu.SMEM)
HB = pl.BlockSpec(memory_space=pltpu.HBM)


def room(mib):
    return pltpu.CompilerParams(vmem_limit_bytes=mib * 2**20)


def cost(flops):
    return pl.CostEstimate(flops=flops, bytes_accessed=10**6, transcendentals=0)


def loop(count, body):
    def step(i, carry):
        body(i)
        return carry

    lax.fori_loop(0, count, step, 0)


def pieces(count, size, body):
    loop(count // size, lambda i: body(pl.ds(pl.multiple_of(i * size, size), size)))


def pick(owner, keys, held, wide, out, stage):
    chunks = keys.shape[0]
    cap = chunks * LANES

    def body(chunk):
        first = chunk * LANES
        for u in range(LANES):
            key = keys[chunk, owner, u]
            stage[pl.ds(first + u, 1), :] = wide[pl.ds(key, 1), :]

    loop(chunks, body)

    def narrow(rows):
        out[rows, :] = stage[rows, :].astype(jnp.bfloat16)

    pieces(cap, LANES, narrow)
    target = held[owner]
    upper = target >> 7
    out[cap : cap + SPARE, :] = upper.astype(jnp.float32).astype(jnp.bfloat16)
    lower = target - upper * LANES
    out[cap + SPARE : cap + 2 * SPARE, :] = lower.astype(jnp.float32).astype(jnp.bfloat16)


def first_pick_kernel(
    hop, unused, place, keys, keys_in, targets, flat, out, wide, held, kept, stage
):
    chunks, owners, _ = targets.shape
    slots = lax.broadcasted_iota(jnp.int32, (chunks, LANES), 0) * LANES
    slots = slots + lax.broadcasted_iota(jnp.int32, (chunks, LANES), 1)
    kept[...] = keys_in[...]
    for owner in range(owners):
        held[owner] = jnp.where(slots < place[2 + owner], targets[:, owner, :], unused)

    def widen(rows):
        wide[rows, :] = flat[rows, :].astype(jnp.float32)

    pieces(flat.shape[0], LANES, widen)
    pick(lax.rem(place[0] + hop, owners), keys, held, wide, out, stage)


def first_pick(hop, unused, place, keys, targets, flat):
    chunks, owners, _ = keys.shape
    cap = chunks * LANES
    width = flat.shape[1]
    return pl.pallas_call(
        functools.partial(first_pick_kernel, hop, unused),
        out_shape=(
            jax.ShapeDtypeStruct((cap + 2 * SPARE, width), jnp.bfloat16),
            jax.ShapeDtypeStruct(flat.shape, jnp.float32),
            jax.ShapeDtypeStruct((owners, chunks, LANES), jnp.int32),
            jax.ShapeDtypeStruct(keys.shape, jnp.int32),
        ),
        in_specs=[SM, SM, VM, VM, VM],
        out_specs=(VM, VM, VM, VM),
        scratch_shapes=[pltpu.VMEM((cap, width), jnp.float32)],
        compiler_params=room(6),
        cost_estimate=cost(10**7),
        name="first_pick",
    )(place, keys, keys, targets, flat)


def pick_kernel(hops, place, keys, held, wide, *refs):
    outs, stages = refs[: len(hops)], refs[len(hops) :]
    owners = held.shape[0]
    for hop, out, stage in zip(hops, outs, stages):
        pick(lax.rem(place[0] + hop, owners), keys, held, wide, out, stage)


def pick_rows(hops, place, keys, held, wide):
    cap = keys.shape[0] * LANES
    width = wide.shape[1]
    shape = jax.ShapeDtypeStruct((cap + 2 * SPARE, width), jnp.bfloat16)
    return pl.pallas_call(
        functools.partial(pick_kernel, hops),
        out_shape=(shape,) * len(hops),
        in_specs=[SM, SM, VM, VM],
        out_specs=(VM,) * len(hops),
        scratch_shapes=[pltpu.VMEM((cap, width), jnp.float32)] * len(hops),
        compiler_params=room(6),
        cost_estimate=cost(10**7 * len(hops)),
        name="pick",
    )(place, keys, held, wide)


def add_rows(pairs, sums, wides, keys, rows, chunk):
    first = chunk * LANES
    for u in range(0, LANES, 2 * pairs):
        for k, row in enumerate(rows):
            for p in range(pairs):
                at, total = u + 2 * p, sums[k * pairs + p]
                one, two = keys[row + chunk, at], keys[row + chunk, at + 1]
                here, next_ = pl.ds(one, 1), pl.ds(two, 1)
                again = jnp.where(one == two, 1.0, 0.0)
                lead = wides[k][pl.ds(first + at, 1), :]
                tail = wides[k][pl.ds(first + at + 1, 1), :] + lead * again
                before, after = total[here, :], total[next_, :]
                total[here, :] = before + lead
                total[next_, :] = after + tail


def prepare(grads, cap, sums, wides, found, keys, sem):
    chunks = cap // LANES
    for k, grad in enumerate(grads):
        upper = grad[cap : cap + SPARE, :].astype(jnp.float32)
        lower = grad[cap + SPARE : cap + 2 * SPARE, :].astype(jnp.float32)
        found[k * chunks : (k + 1) * chunks, :] = (upper * LANES + lower).astype(jnp.int32)
    copy = pltpu.make_async_copy(found, keys, sem)
    copy.start()

    def widen(rows):
        for wide, grad in zip(wides, grads):
            wide[rows, :] = grad[rows, :].astype(jnp.float32)

    def clear(rows):
        for total in sums:
            total[rows, :] = jnp.zeros((64, LANES), jnp.float32)

    pieces(cap, 64, widen)
    pieces(sums[0].shape[0] // 64 * 64, 64, clear)
    copy.wait()


def own_kernel(parts, place, keys, held, wide, out, *refs):
    sums, (found, sem) = refs[:parts], refs[parts:]
    owner = place[0]
    copy = pltpu.make_async_copy(held.at[owner], found, sem)
    copy.start()

    def clear(rows):
        for total in sums:
            total[rows, :] = jnp.zeros((64, LANES), jnp.float32)

    pieces(sums[0].shape[0] // 64 * 64, 64, clear)
    copy.wait()

    def body(chunk):
        for u in range(0, LANES, 2 * parts):
            for p, total in enumerate(sums):
                at = u + 2 * p
                one, two = found[chunk, at], found[chunk, at + 1]
                lead = wide[pl.ds(keys[chunk, owner, at], 1), :]
                tail = wide[pl.ds(keys[chunk, owner, at + 1], 1), :]
                tail = tail + lead * jnp.where(one == two, 1.0, 0.0)
                here, next_ = pl.ds(one, 1), pl.ds(two, 1)
                before, after = total[here, :], total[next_, :]
                total[here, :] = before + lead
                total[next_, :] = after + tail

    loop(keys.shape[0], body)

    def add_up(rows):
        total = sums[0][rows, :]
        for part in sums[1:]:
            total = total + part[rows, :]
        out[rows, :] = total

    pieces(out.shape[0], 64, add_up)


def scatter_kernel(cap, senders, place, begun, *refs):
    grads, outs, refs = refs[:senders], refs[senders : senders + 2], refs[senders + 2 :]
    sums, wides = refs[:senders], refs[senders : 2 * senders]
    found, keys, sem = refs[2 * senders :]
    chunks = cap // LANES
    prepare(grads, cap, sums, wides, found, keys, sem)
    rows = [k * chunks for k in range(senders)]
    loop(chunks, lambda chunk: add_rows(1, sums, wides, keys, rows, chunk))
    half = outs[0].shape[0]
    for out, index in ((outs[1], 1 - place[1]), (outs[0], place[1])):

        def add_up(i):
            there = pl.ds(pl.multiple_of(index * half + i * 64, 64), 64)
            total = begun[there, :]
            for part in sums:
                total = total + part[there, :]
            out[pl.ds(pl.multiple_of(i * 64, 64), 64), :] = total

        loop(half // 64, add_up)


def tables_of(rows, width, cap, senders, pairs):
    chunks = cap // LANES
    return (
        [pltpu.VMEM((rows + SPARE, width), jnp.float32)] * (senders * pairs)
        + [pltpu.VMEM((cap, width), jnp.float32)] * senders
        + [
            pltpu.VMEM((senders * chunks, LANES), jnp.int32),
            pltpu.SMEM((senders * chunks, LANES), jnp.int32),
            pltpu.SemaphoreType.DMA,
        ]
    )


def own_rows(place, keys, held, wide, rows):
    width = wide.shape[1]
    parts = 2
    return pl.pallas_call(
        functools.partial(own_kernel, parts),
        out_shape=jax.ShapeDtypeStruct((rows, width), jnp.float32),
        in_specs=[SM, SM, VM, VM],
        out_specs=VM,
        scratch_shapes=[pltpu.VMEM((rows + SPARE, width), jnp.float32)] * parts
        + [pltpu.SMEM(held.shape[1:], jnp.int32), pltpu.SemaphoreType.DMA],
        compiler_params=room(16),
        cost_estimate=cost(10**7),
        name="own_rows",
    )(place, keys, held, wide)


def scatter_add(place, begun, grads):
    senders = len(grads)
    cap, width = grads[0].shape[0] - 2 * SPARE, grads[0].shape[1]
    rows = begun.shape[0]
    shape = jax.ShapeDtypeStruct((rows // 2, width), jnp.float32)
    return pl.pallas_call(
        functools.partial(scatter_kernel, cap, senders),
        out_shape=(shape, shape),
        in_specs=[SM, VM] + [VM] * senders,
        out_specs=(VM, VM),
        scratch_shapes=tables_of(rows, width, cap, senders, 1),
        compiler_params=room(24),
        cost_estimate=cost(10**8),
        name="scatter",
    )(place, begun, *grads)


def diagonal():
    lane = lax.broadcasted_iota(jnp.int32, (LANES, LANES), 1)
    return lax.broadcasted_iota(jnp.int32, (LANES, LANES), 0) == lane


def to_row(column, diag):
    return jnp.sum(jnp.where(diag, column, 0.0), axis=0, keepdims=True)


def to_column(row, diag):
    return jnp.sum(jnp.where(diag, row, 0.0), axis=1, keepdims=True)


def powers_of(peaks):
    return jnp.ceil(STEPS * jnp.log2(jnp.maximum(peaks, TINY) / TOP))


def short(x):
    return x.astype(jnp.int32).astype(jnp.int16)


def wide_of(x):
    return x.astype(jnp.int32).astype(jnp.float32)


def rounded(x):
    return short((x + ROUNDER) - ROUNDER)


def encode_blocks(block, put, count, peaks, shrinks, diag):
    for k in range(count):
        peak = jnp.max(jnp.abs(block(k)), axis=1, keepdims=True)
        peaks[k : k + 1, :] = to_row(peak, diag)
    powers = powers_of(peaks[...])
    peaks[...] = powers
    shrinks[...] = jnp.exp2(powers * (-1.0 / STEPS))
    for k in range(count):
        tail = short(jnp.broadcast_to(peaks[k : k + 1, :], (SPARE, LANES)))
        put(k, rounded(block(k) * to_column(shrinks[k : k + 1, :], diag)), tail)


def decode(part, diag):
    scale = to_column(jnp.exp2(wide_of(part[LANES:CODED]) * (1.0 / STEPS))[0:1], diag)
    return wide_of(part[0:LANES]) * scale


def encode_kernel(together, mine, got, out, peaks, shrinks):
    diag = diagonal()
    groups, blocks = out.shape[:2]
    size = blocks * LANES

    def body(step, carry):
        def at(i):
            return step * together + i // blocks, i % blocks

        def block(i):
            group, k = at(i)
            rows = pl.ds(pl.multiple_of(group * size + k * LANES, LANES), LANES)
            return mine[rows, :] + got[rows, :]

        def put(i, code, tail):
            group, k = at(i)
            out[group, k, 0:LANES, :] = code
            out[group, k, LANES:CODED, :] = tail

        encode_blocks(block, put, together * blocks, peaks, shrinks, diag)
        return carry

    lax.fori_loop(0, groups // together, body, 0)


def encode_sum(mine, got, groups):
    blocks = mine.shape[0] // (groups * LANES)
    together = 2
    return pl.pallas_call(
        functools.partial(encode_kernel, together),
        out_shape=jax.ShapeDtypeStruct((groups, blocks, CODED, LANES), jnp.int16),
        in_specs=[VM, VM],
        out_specs=VM,
        scratch_shapes=[pltpu.VMEM((together * blocks, LANES), jnp.float32)] * 2,
        compiler_params=room(8),
        cost_estimate=cost(10**7),
        name="encode",
    )(mine, got)


def first_sum_kernel(parts, out, totals, peaks, shrinks):
    diag = diagonal()
    groups, blocks = parts.shape[:2]

    def body(k, carry):
        total = decode(parts[0, k], diag)
        for j in range(1, groups):
            total = total + decode(parts[j, k], diag)
        totals[k] = total
        return carry

    lax.fori_loop(0, blocks, body, 0)

    def put(k, code, tail):
        out[k, 0:LANES, :] = code
        out[k, LANES:CODED, :] = tail

    encode_blocks(lambda k: totals[k], put, blocks, peaks, shrinks, diag)


def first_sum(parts):
    blocks = parts.shape[1]
    return pl.pallas_call(
        first_sum_kernel,
        out_shape=jax.ShapeDtypeStruct(parts.shape[1:], jnp.int16),
        in_specs=[VM],
        out_specs=VM,
        scratch_shapes=[pltpu.VMEM((blocks, LANES, LANES), jnp.float32)]
        + [pltpu.VMEM((blocks, LANES), jnp.float32)] * 2,
        compiler_params=room(6),
        cost_estimate=cost(10**7),
        name="first_sum",
    )(parts)


def last_sum_kernel(parts, out):
    diag = diagonal()
    total = decode(parts[0], diag)
    for j in range(1, parts.shape[0]):
        total = total + decode(parts[j], diag)
    powers = powers_of(to_row(jnp.max(jnp.abs(total), axis=1, keepdims=True), diag))
    code = rounded(total * to_column(jnp.exp2(powers * (-1.0 / STEPS)), diag))
    tail = short(jnp.broadcast_to(powers, (SPARE, LANES)))
    for j in range(out.shape[0]):
        out[j, 0:LANES, :] = code
        out[j, LANES:CODED, :] = tail


def last_sum(parts):
    return pl.pallas_call(
        last_sum_kernel,
        out_shape=jax.ShapeDtypeStruct(parts.shape, jnp.int16),
        in_specs=[VM],
        out_specs=VM,
        compiler_params=room(4),
        cost_estimate=cost(10**6),
        name="last_sum",
    )(parts)


def update_kernel(count, groups, core, *refs):
    mine, got = refs[:count], refs[count : 2 * count]
    rows, state = refs[2 * count : 2 * count + 2]
    new_rows, new_state, held, sums, scales = refs[-5:]
    step = pl.program_id(0)
    tables, blocks = held.shape[:2]
    size = blocks * LANES
    for d in range(count):

        @pl.when(step == d)
        def _():
            held[core[0]] = mine[d][...]
            held[1 - core[0]] = got[d][...]

    diag = diagonal()
    start = groups[step] * size
    every = [(table, k) for table in range(tables) for k in range(blocks)]
    for at, (table, k) in enumerate(every):
        code = wide_of(held[table, k, 0:LANES, :])
        sums[at : at + 1, :] = to_row(jnp.sum(code * code, axis=1, keepdims=True), diag)
        scales[at : at + 1, :] = wide_of(held[table, k, LANES:CODED, :])[0:1]
    scale = jnp.exp2(scales[...] * (1.0 / STEPS))
    gain = sums[...] * (scale * scale) * (1.0 / LANES)
    for at, (table, k) in enumerate(every):
        lanes = slice(k * LANES, (k + 1) * LANES)
        there = pl.ds(pl.multiple_of(start + k * LANES, LANES), LANES)
        updated = state[table : table + 1, there] + gain[at : at + 1, :]
        new_state[table : table + 1, lanes] = updated
        sums[at : at + 1, :] = updated
    scales[...] = LEARN_RATE * scale / (jnp.sqrt(sums[...]) + EPSILON)
    for at, (table, k) in enumerate(every):
        there = slice(k * LANES, (k + 1) * LANES)
        move = wide_of(held[table, k, 0:LANES, :]) * to_column(scales[at : at + 1, :], diag)
        new_rows[table, there, :] = rows[step, table, there, :] - move


def update(groups, core, mine, got, rows, state, earlier):
    count, tables, size, width = rows.shape
    blocks = mine[0].shape[0]
    row_spec = pl.BlockSpec((tables, size, width), lambda i, g, c: (0, g[i], 0))
    state_spec = pl.BlockSpec((tables, size), lambda i, g, c: (0, g[i]))
    first = 2 + 2 * count + 2
    return pl.pallas_call(
        functools.partial(update_kernel, count),
        grid_spec=pltpu.PrefetchScalarGridSpec(
            num_scalar_prefetch=2,
            grid=(count,),
            in_specs=[VM] * (2 * count) + [VM, VM] + [HB] * len(earlier),
            out_specs=(row_spec, state_spec),
            scratch_shapes=[
                pltpu.VMEM((tables, *mine[0].shape), jnp.int16),
            ]
            + [pltpu.VMEM((tables * blocks, LANES), jnp.float32)] * 2,
        ),
        out_shape=(
            jax.ShapeDtypeStruct((tables, state.shape[1], width), jnp.float32),
            jax.ShapeDtypeStruct(state.shape, jnp.float32),
        ),
        input_output_aliases={first: 0, first + 1: 1} if earlier else {},
        compiler_params=room(12),
        cost_estimate=cost(10**7),
        name="update",
    )(groups, core, *mine, *got, rows, state, *earlier)


def fetch_kernel(groups, rows, after, *refs):
    outs, sems = refs[:-1], refs[-1]
    count, _, size, _ = outs[0].shape
    copies = []
    for i, out in enumerate(outs):
        for d in range(count):
            at = i * count + d
            there = pl.ds(pl.multiple_of(groups[at] * size, size), size)
            copies.append(pltpu.make_async_copy(rows.at[:, there, :], out.at[d], sems.at[at]))
    for copy in copies:
        copy.start()
    for copy in copies:
        copy.wait()


def fetch(groups, rows, after):
    tables, rows_dev, width = rows.shape
    count = groups.shape[0]
    shape = jax.ShapeDtypeStruct((count // 2, tables, rows_dev // count, width), rows.dtype)
    return pl.pallas_call(
        fetch_kernel,
        out_shape=(shape, shape),
        in_specs=[SM, HB, HB],
        out_specs=(VM, VM),
        scratch_shapes=[pltpu.SemaphoreType.DMA((count,))],
        compiler_params=room(5),
        cost_estimate=cost(3 * 10**7),
        name="fetch",
    )(groups, rows, after)


def keep_kernel(state, out):
    out[...] = state[...]


def keep(state):
    return pl.pallas_call(
        keep_kernel,
        out_shape=jax.ShapeDtypeStruct(state.shape, state.dtype),
        in_specs=[VM],
        out_specs=VM,
        compiler_params=room(1),
        cost_estimate=cost(10**5),
        name="keep",
    )(state)


def shift(x, axis, by):
    count = lax.axis_size(axis)
    return lax.ppermute(x, axis, [(i, (i + by) % count) for i in range(count)])


def square_shift(x, pair_by, ring_by):
    pairs, rings = lax.axis_size("pair"), lax.axis_size("ring")
    links = [
        (p * rings + r, (p + pair_by) % pairs * rings + (r + ring_by) % rings)
        for p in range(pairs)
        for r in range(rings)
    ]
    return lax.ppermute(x, SQUARE, links)


def lane_view(slots):
    owners, cap = slots.shape[1:]
    return slots.reshape(owners, cap // LANES, LANES).transpose(1, 0, 2)


def shards(pooled_grad, slot_source, slot_target, slot_count, table_rows, accum):
    feature = pooled_grad.shape[2]
    tables, rows_dev, _ = table_rows.shape
    pairs, rings = lax.axis_size("pair"), lax.axis_size("ring")
    row, core, pair, ring = (lax.axis_index(a) for a in ("rows", "core", "pair", "ring"))
    hops = [(0, 0), (0, 1), (0, 3), (1, 0), (1, 1), (1, 3), (0, 2), (1, 2)]
    behind = [(pair + p) % pairs * rings + (ring + rings - r) % rings for p, r in hops]
    place = jnp.concatenate([jnp.stack([row, core]).astype(jnp.int32), slot_count[0]])
    core = core.astype(jnp.int32).reshape(1)
    flat_grad = pooled_grad.reshape(-1, feature)
    keys, targets = lane_view(slot_source), lane_view(slot_target)

    rows = tables * rows_dev
    first, wide, held, keys = first_pick(2, rows, place, keys, targets, flat_grad)
    picked = {2: first}
    picked.update(zip((1, 3), pick_rows((1, 3), place, keys, held, wide)))
    grads = []
    for hop, block in picked.items():
        grads.append(shift(block, "rows", hop))
    begun = own_rows(place, keys, held, wide, rows)
    mine, other = scatter_add(place, begun, grads)
    order = ((7, 6, 5, 0), (4, 3, 2, 1))
    behind = jnp.stack([behind[d] for part in order for d in part]).astype(jnp.int32)
    fetched = fetch(behind, table_rows, begun)
    got = shift(other, "core", 1)
    coded = encode_sum(mine, got, pairs * rings)
    parts = lax.all_to_all(coded, SQUARE, 0, 0, tiled=True)
    parts = lax.all_to_all(first_sum(parts), "far", 0, 0, tiled=True)
    bundle = lax.all_to_all(last_sum(parts), "far", 0, 0, tiled=True)
    whole = [None] * len(hops)
    for d in reversed(range(len(hops))):
        whole[d] = square_shift(bundle, *hops[d]) if d else bundle
    state = keep(accum)
    swapped = [shift(w, "core", 1) for w in whole]
    result = ()
    for i in range(2):
        result = update(
            behind[4 * i : 4 * i + 4],
            core,
            [whole[d] for d in order[i]],
            [swapped[d] for d in order[i]],
            fetched[i],
            state,
            result,
        )
    return result


def solution(mesh):
    split = Mesh(mesh.devices.reshape(4, 2, 4, 2, mesh.shape["rows"]), AXES)
    placed = (
        P(AXES, None, None),
        P(AXES, None, None),
        P(AXES, None, None),
        P(AXES, None),
        P(None, "rows", None),
        P(None, "rows"),
    )

    return jax.shard_map(
        shards,
        mesh=split,
        in_specs=placed,
        out_specs=(P(None, "rows", None), P(None, "rows")),
        check_vma=False,
    )
```

```python
import functools

import jax
import jax.numpy as jnp
from jax import lax
from jax.experimental import pallas as pl
from jax.experimental.pallas import tpu as pltpu
from jax.sharding import Mesh
from jax.sharding import PartitionSpec as P


AXES = ("far", "pair", "ring", "core", "rows")
SQUARE = ("pair", "ring")

LEARN_RATE = 0.1
EPSILON = 1e-06
LANES = 128
SPARE = 8
CODED = LANES + SPARE
STEPS = 64.0
TOP = 32700.0
TINY = 1e-30
ROUNDER = 12582912.0

VM = pl.BlockSpec(memory_space=pltpu.VMEM)
SM = pl.BlockSpec(memory_space=pltpu.SMEM)
HB = pl.BlockSpec(memory_space=pltpu.HBM)


def room(mib):
    return pltpu.CompilerParams(vmem_limit_bytes=mib * 2**20)


def cost(flops):
    return pl.CostEstimate(flops=flops, bytes_accessed=10**6, transcendentals=0)


def loop(count, body):
    def step(i, carry):
        body(i)
        return carry

    lax.fori_loop(0, count, step, 0)


def pieces(count, size, body):
    loop(count // size, lambda i: body(pl.ds(pl.multiple_of(i * size, size), size)))


def pick(owner, keys, held, wide, out, stage):
    chunks = keys.shape[0]
    cap = chunks * LANES

    def body(chunk):
        first = chunk * LANES
        for u in range(LANES):
            key = keys[chunk, owner, u]
            stage[pl.ds(first + u, 1), :] = wide[pl.ds(key, 1), :]

    loop(chunks, body)

    def narrow(rows):
        out[rows, :] = stage[rows, :].astype(jnp.bfloat16)

    pieces(cap, LANES, narrow)
    target = held[owner]
    upper = target >> 7
    out[cap : cap + SPARE, :] = upper.astype(jnp.float32).astype(jnp.bfloat16)
    lower = target - upper * LANES
    out[cap + SPARE : cap + 2 * SPARE, :] = lower.astype(jnp.float32).astype(jnp.bfloat16)


def first_pick_kernel(
    hop, unused, place, keys, keys_in, targets, flat, out, wide, held, kept, stage
):
    chunks, owners, _ = targets.shape
    slots = lax.broadcasted_iota(jnp.int32, (chunks, LANES), 0) * LANES
    slots = slots + lax.broadcasted_iota(jnp.int32, (chunks, LANES), 1)
    kept[...] = keys_in[...]
    for owner in range(owners):
        held[owner] = jnp.where(slots < place[2 + owner], targets[:, owner, :], unused)

    def widen(rows):
        wide[rows, :] = flat[rows, :].astype(jnp.float32)

    pieces(flat.shape[0], LANES, widen)
    pick(lax.rem(place[0] + hop, owners), keys, held, wide, out, stage)


def first_pick(hop, unused, place, keys, targets, flat):
    chunks, owners, _ = keys.shape
    cap = chunks * LANES
    width = flat.shape[1]
    return pl.pallas_call(
        functools.partial(first_pick_kernel, hop, unused),
        out_shape=(
            jax.ShapeDtypeStruct((cap + 2 * SPARE, width), jnp.bfloat16),
            jax.ShapeDtypeStruct(flat.shape, jnp.float32),
            jax.ShapeDtypeStruct((owners, chunks, LANES), jnp.int32),
            jax.ShapeDtypeStruct(keys.shape, jnp.int32),
        ),
        in_specs=[SM, SM, VM, VM, VM],
        out_specs=(VM, VM, VM, VM),
        scratch_shapes=[pltpu.VMEM((cap, width), jnp.float32)],
        compiler_params=room(6),
        cost_estimate=cost(10**7),
        name="first_pick",
    )(place, keys, keys, targets, flat)


def pick_kernel(hops, place, keys, held, wide, *refs):
    outs, stages = refs[: len(hops)], refs[len(hops) :]
    owners = held.shape[0]
    for hop, out, stage in zip(hops, outs, stages):
        pick(lax.rem(place[0] + hop, owners), keys, held, wide, out, stage)


def pick_rows(hops, place, keys, held, wide):
    cap = keys.shape[0] * LANES
    width = wide.shape[1]
    shape = jax.ShapeDtypeStruct((cap + 2 * SPARE, width), jnp.bfloat16)
    return pl.pallas_call(
        functools.partial(pick_kernel, hops),
        out_shape=(shape,) * len(hops),
        in_specs=[SM, SM, VM, VM],
        out_specs=(VM,) * len(hops),
        scratch_shapes=[pltpu.VMEM((cap, width), jnp.float32)] * len(hops),
        compiler_params=room(6),
        cost_estimate=cost(10**7 * len(hops)),
        name="pick",
    )(place, keys, held, wide)


def add_rows(pairs, sums, wides, keys, rows, chunk):
    first = chunk * LANES
    for u in range(0, LANES, 2 * pairs):
        for k, row in enumerate(rows):
            for p in range(pairs):
                at, total = u + 2 * p, sums[k * pairs + p]
                one, two = keys[row + chunk, at], keys[row + chunk, at + 1]
                here, next_ = pl.ds(one, 1), pl.ds(two, 1)
                again = jnp.where(one == two, 1.0, 0.0)
                lead = wides[k][pl.ds(first + at, 1), :]
                tail = wides[k][pl.ds(first + at + 1, 1), :] + lead * again
                before, after = total[here, :], total[next_, :]
                total[here, :] = before + lead
                total[next_, :] = after + tail


def prepare(grads, cap, sums, wides, found, keys, sem):
    chunks = cap // LANES
    for k, grad in enumerate(grads):
        upper = grad[cap : cap + SPARE, :].astype(jnp.float32)
        lower = grad[cap + SPARE : cap + 2 * SPARE, :].astype(jnp.float32)
        found[k * chunks : (k + 1) * chunks, :] = (upper * LANES + lower).astype(jnp.int32)
    copy = pltpu.make_async_copy(found, keys, sem)
    copy.start()

    def widen(rows):
        for wide, grad in zip(wides, grads):
            wide[rows, :] = grad[rows, :].astype(jnp.float32)

    def clear(rows):
        for total in sums:
            total[rows, :] = jnp.zeros((64, LANES), jnp.float32)

    pieces(cap, 64, widen)
    pieces(sums[0].shape[0] // 64 * 64, 64, clear)
    copy.wait()


def own_kernel(parts, place, keys, held, wide, out, *refs):
    sums, (found, sem) = refs[:parts], refs[parts:]
    owner = place[0]
    copy = pltpu.make_async_copy(held.at[owner], found, sem)
    copy.start()

    def clear(rows):
        for total in sums:
            total[rows, :] = jnp.zeros((64, LANES), jnp.float32)

    pieces(sums[0].shape[0] // 64 * 64, 64, clear)
    copy.wait()

    def body(chunk):
        for u in range(0, LANES, 2 * parts):
            for p, total in enumerate(sums):
                at = u + 2 * p
                one, two = found[chunk, at], found[chunk, at + 1]
                lead = wide[pl.ds(keys[chunk, owner, at], 1), :]
                tail = wide[pl.ds(keys[chunk, owner, at + 1], 1), :]
                tail = tail + lead * jnp.where(one == two, 1.0, 0.0)
                here, next_ = pl.ds(one, 1), pl.ds(two, 1)
                before, after = total[here, :], total[next_, :]
                total[here, :] = before + lead
                total[next_, :] = after + tail

    loop(keys.shape[0], body)

    def add_up(rows):
        total = sums[0][rows, :]
        for part in sums[1:]:
            total = total + part[rows, :]
        out[rows, :] = total

    pieces(out.shape[0], 64, add_up)


def scatter_kernel(cap, senders, place, begun, *refs):
    grads, outs, refs = refs[:senders], refs[senders : senders + 2], refs[senders + 2 :]
    sums, wides = refs[:senders], refs[senders : 2 * senders]
    found, keys, sem = refs[2 * senders :]
    chunks = cap // LANES
    prepare(grads, cap, sums, wides, found, keys, sem)
    rows = [k * chunks for k in range(senders)]
    loop(chunks, lambda chunk: add_rows(1, sums, wides, keys, rows, chunk))
    half = outs[0].shape[0]
    for out, index in ((outs[1], 1 - place[1]), (outs[0], place[1])):

        def add_up(i):
            there = pl.ds(pl.multiple_of(index * half + i * 64, 64), 64)
            total = begun[there, :]
            for part in sums:
                total = total + part[there, :]
            out[pl.ds(pl.multiple_of(i * 64, 64), 64), :] = total

        loop(half // 64, add_up)


def tables_of(rows, width, cap, senders, pairs):
    chunks = cap // LANES
    return (
        [pltpu.VMEM((rows + SPARE, width), jnp.float32)] * (senders * pairs)
        + [pltpu.VMEM((cap, width), jnp.float32)] * senders
        + [
            pltpu.VMEM((senders * chunks, LANES), jnp.int32),
            pltpu.SMEM((senders * chunks, LANES), jnp.int32),
            pltpu.SemaphoreType.DMA,
        ]
    )


def own_rows(place, keys, held, wide, rows):
    width = wide.shape[1]
    parts = 2
    return pl.pallas_call(
        functools.partial(own_kernel, parts),
        out_shape=jax.ShapeDtypeStruct((rows, width), jnp.float32),
        in_specs=[SM, SM, VM, VM],
        out_specs=VM,
        scratch_shapes=[pltpu.VMEM((rows + SPARE, width), jnp.float32)] * parts
        + [pltpu.SMEM(held.shape[1:], jnp.int32), pltpu.SemaphoreType.DMA],
        compiler_params=room(16),
        cost_estimate=cost(10**7),
        name="own_rows",
    )(place, keys, held, wide)


def scatter_add(place, begun, grads):
    senders = len(grads)
    cap, width = grads[0].shape[0] - 2 * SPARE, grads[0].shape[1]
    rows = begun.shape[0]
    shape = jax.ShapeDtypeStruct((rows // 2, width), jnp.float32)
    return pl.pallas_call(
        functools.partial(scatter_kernel, cap, senders),
        out_shape=(shape, shape),
        in_specs=[SM, VM] + [VM] * senders,
        out_specs=(VM, VM),
        scratch_shapes=tables_of(rows, width, cap, senders, 1),
        compiler_params=room(24),
        cost_estimate=cost(10**8),
        name="scatter",
    )(place, begun, *grads)


def diagonal():
    lane = lax.broadcasted_iota(jnp.int32, (LANES, LANES), 1)
    return lax.broadcasted_iota(jnp.int32, (LANES, LANES), 0) == lane


def to_row(column, diag):
    return jnp.sum(jnp.where(diag, column, 0.0), axis=0, keepdims=True)


def to_column(row, diag):
    return jnp.sum(jnp.where(diag, row, 0.0), axis=1, keepdims=True)


def powers_of(peaks):
    return jnp.ceil(STEPS * jnp.log2(jnp.maximum(peaks, TINY) / TOP))


def short(x):
    return x.astype(jnp.int32).astype(jnp.int16)


def wide_of(x):
    return x.astype(jnp.int32).astype(jnp.float32)


def rounded(x):
    return short((x + ROUNDER) - ROUNDER)


def encode_blocks(block, put, count, peaks, shrinks, diag):
    for k in range(count):
        peak = jnp.max(jnp.abs(block(k)), axis=1, keepdims=True)
        peaks[k : k + 1, :] = to_row(peak, diag)
    powers = powers_of(peaks[...])
    peaks[...] = powers
    shrinks[...] = jnp.exp2(powers * (-1.0 / STEPS))
    for k in range(count):
        tail = short(jnp.broadcast_to(peaks[k : k + 1, :], (SPARE, LANES)))
        put(k, rounded(block(k) * to_column(shrinks[k : k + 1, :], diag)), tail)


def decode(part, diag):
    scale = to_column(jnp.exp2(wide_of(part[LANES:CODED]) * (1.0 / STEPS))[0:1], diag)
    return wide_of(part[0:LANES]) * scale


def encode_kernel(offset, targets, mine, got, *refs):
    outs, (peaks, shrinks) = refs[:-2], refs[-2:]
    diag = diagonal()
    blocks = outs[0].shape[0]
    together = peaks.shape[0] // blocks
    size = blocks * LANES
    for low in range(0, len(outs), together):
        some = outs[low : low + together]

        def block(i, low=low):
            first = targets[offset + low + i // blocks] * size + i % blocks * LANES
            rows = pl.ds(pl.multiple_of(first, LANES), LANES)
            return mine[rows, :] + got[rows, :]

        def put(i, code, tail, some=some):
            out, k = some[i // blocks], i % blocks
            out[k, 0:LANES, :] = code
            out[k, LANES:CODED, :] = tail

        encode_blocks(block, put, len(some) * blocks, peaks, shrinks, diag)


def encode_sum(offset, count, targets, mine, got, groups):
    blocks = mine.shape[0] // (groups * LANES)
    shape = jax.ShapeDtypeStruct((blocks, CODED, LANES), jnp.int16)
    return pl.pallas_call(
        functools.partial(encode_kernel, offset),
        out_shape=(shape,) * count,
        in_specs=[SM, VM, VM],
        out_specs=(VM,) * count,
        scratch_shapes=[pltpu.VMEM((2 * blocks, LANES), jnp.float32)] * 2,
        compiler_params=room(8),
        cost_estimate=cost(10**7),
        name="encode",
    )(targets, mine, got)


def first_sum_kernel(*refs):
    parts, (out, totals, peaks, shrinks) = refs[:-4], refs[-4:]
    diag = diagonal()
    blocks = out.shape[0]

    def body(k, carry):
        total = decode(parts[0][k], diag)
        for part in parts[1:]:
            total = total + decode(part[k], diag)
        totals[k] = total
        return carry

    lax.fori_loop(0, blocks, body, 0)

    def put(k, code, tail):
        out[k, 0:LANES, :] = code
        out[k, LANES:CODED, :] = tail

    encode_blocks(lambda k: totals[k], put, blocks, peaks, shrinks, diag)


def first_sum(parts):
    blocks = parts[0].shape[0]
    return pl.pallas_call(
        first_sum_kernel,
        out_shape=jax.ShapeDtypeStruct(parts[0].shape, jnp.int16),
        in_specs=[VM] * len(parts),
        out_specs=VM,
        scratch_shapes=[pltpu.VMEM((blocks, LANES, LANES), jnp.float32)]
        + [pltpu.VMEM((blocks, LANES), jnp.float32)] * 2,
        compiler_params=room(6),
        cost_estimate=cost(10**7),
        name="first_sum",
    )(*parts)


def last_sum_kernel(parts, out):
    diag = diagonal()
    total = decode(parts[0], diag)
    for j in range(1, parts.shape[0]):
        total = total + decode(parts[j], diag)
    powers = powers_of(to_row(jnp.max(jnp.abs(total), axis=1, keepdims=True), diag))
    code = rounded(total * to_column(jnp.exp2(powers * (-1.0 / STEPS)), diag))
    tail = short(jnp.broadcast_to(powers, (SPARE, LANES)))
    for j in range(out.shape[0]):
        out[j, 0:LANES, :] = code
        out[j, LANES:CODED, :] = tail


def last_sum(parts):
    return pl.pallas_call(
        last_sum_kernel,
        out_shape=jax.ShapeDtypeStruct(parts.shape, jnp.int16),
        in_specs=[VM],
        out_specs=VM,
        compiler_params=room(4),
        cost_estimate=cost(10**6),
        name="last_sum",
    )(parts)


def update_kernel(count, offset, groups, core, *refs):
    mine, got = refs[:count], refs[count : 2 * count]
    rows, state = refs[2 * count : 2 * count + 2]
    new_rows, new_state, held, sums, scales = refs[-5:]
    step = pl.program_id(0)
    tables, blocks = held.shape[:2]
    size = blocks * LANES
    for d in range(count):

        @pl.when(step == d)
        def _():
            held[core[0]] = mine[d][...]
            held[1 - core[0]] = got[d][...]

    diag = diagonal()
    start = groups[offset + step] * size
    every = [(table, k) for table in range(tables) for k in range(blocks)]
    for at, (table, k) in enumerate(every):
        code = wide_of(held[table, k, 0:LANES, :])
        sums[at : at + 1, :] = to_row(jnp.sum(code * code, axis=1, keepdims=True), diag)
        scales[at : at + 1, :] = wide_of(held[table, k, LANES:CODED, :])[0:1]
    scale = jnp.exp2(scales[...] * (1.0 / STEPS))
    gain = sums[...] * (scale * scale) * (1.0 / LANES)
    for at, (table, k) in enumerate(every):
        lanes = slice(k * LANES, (k + 1) * LANES)
        there = pl.ds(pl.multiple_of(start + k * LANES, LANES), LANES)
        updated = state[table : table + 1, there] + gain[at : at + 1, :]
        new_state[table : table + 1, lanes] = updated
        sums[at : at + 1, :] = updated
    scales[...] = LEARN_RATE * scale / (jnp.sqrt(sums[...]) + EPSILON)
    for at, (table, k) in enumerate(every):
        there = slice(k * LANES, (k + 1) * LANES)
        move = wide_of(held[table, k, 0:LANES, :]) * to_column(scales[at : at + 1, :], diag)
        new_rows[table, there, :] = rows[step, table, there, :] - move


def update(offset, groups, core, mine, got, rows, state, earlier):
    count, tables, size, width = rows.shape
    blocks = mine[0].shape[0]
    row_spec = pl.BlockSpec((tables, size, width), lambda i, g, c: (0, g[offset + i], 0))
    state_spec = pl.BlockSpec((tables, size), lambda i, g, c: (0, g[offset + i]))
    first = 2 + 2 * count + 2
    return pl.pallas_call(
        functools.partial(update_kernel, count, offset),
        grid_spec=pltpu.PrefetchScalarGridSpec(
            num_scalar_prefetch=2,
            grid=(count,),
            in_specs=[VM] * (2 * count) + [VM, VM] + [HB] * len(earlier),
            out_specs=(row_spec, state_spec),
            scratch_shapes=[
                pltpu.VMEM((tables, *mine[0].shape), jnp.int16),
            ]
            + [pltpu.VMEM((tables * blocks, LANES), jnp.float32)] * 2,
        ),
        out_shape=(
            jax.ShapeDtypeStruct((tables, state.shape[1], width), jnp.float32),
            jax.ShapeDtypeStruct(state.shape, jnp.float32),
        ),
        input_output_aliases={first: 0, first + 1: 1} if earlier else {},
        compiler_params=room(12),
        cost_estimate=cost(10**7),
        name="update",
    )(groups, core, *mine, *got, rows, state, *earlier)


def fetch_kernel(groups, rows, after, *refs):
    outs, sems = refs[:-1], refs[-1]
    size = outs[0].shape[2]
    copies = []
    for out in outs:
        for d in range(out.shape[0]):
            at = len(copies)
            there = pl.ds(pl.multiple_of(groups[at] * size, size), size)
            copies.append(pltpu.make_async_copy(rows.at[:, there, :], out.at[d], sems.at[at]))
    for copy in copies:
        copy.start()
    for copy in copies:
        copy.wait()


def fetch(groups, split, count, rows, after):
    tables, rows_dev, width = rows.shape
    shapes = [
        jax.ShapeDtypeStruct((size, tables, rows_dev // count, width), rows.dtype)
        for size in (split, count - split)
    ]
    return pl.pallas_call(
        fetch_kernel,
        out_shape=shapes,
        in_specs=[SM, HB, HB],
        out_specs=(VM, VM),
        scratch_shapes=[pltpu.SemaphoreType.DMA((count,))],
        compiler_params=room(5),
        cost_estimate=cost(3 * 10**7),
        name="fetch",
    )(groups, rows, after)


def keep_kernel(state, out):
    out[...] = state[...]


def keep(state):
    return pl.pallas_call(
        keep_kernel,
        out_shape=jax.ShapeDtypeStruct(state.shape, state.dtype),
        in_specs=[VM],
        out_specs=VM,
        compiler_params=room(1),
        cost_estimate=cost(10**5),
        name="keep",
    )(state)


def shift(x, axis, by):
    count = lax.axis_size(axis)
    return lax.ppermute(x, axis, [(i, (i + by) % count) for i in range(count)])


def square_shift(x, pair_by, ring_by):
    pairs, rings = lax.axis_size("pair"), lax.axis_size("ring")
    links = [
        (p * rings + r, (p + pair_by) % pairs * rings + (r + ring_by) % rings)
        for p in range(pairs)
        for r in range(rings)
    ]
    return lax.ppermute(x, SQUARE, links)


def lane_view(slots):
    owners, cap = slots.shape[1:]
    return slots.reshape(owners, cap // LANES, LANES).transpose(1, 0, 2)


def shards(pooled_grad, slot_source, slot_target, slot_count, table_rows, accum):
    feature = pooled_grad.shape[2]
    tables, rows_dev, _ = table_rows.shape
    pairs, rings = lax.axis_size("pair"), lax.axis_size("ring")
    row, core, pair, ring = (lax.axis_index(a) for a in ("rows", "core", "pair", "ring"))
    hops = [(0, 0), (0, 1), (0, 3), (1, 0), (1, 1), (1, 3), (0, 2), (1, 2)]
    behind = [(pair + p) % pairs * rings + (ring + rings - r) % rings for p, r in hops]
    ahead = [(pair + p) % pairs * rings + (ring + r) % rings for p, r in hops]
    order = ((7, 6, 5, 2, 0), (1, 4, 3))
    sends = ((7, 6, 5), (2, 1, 4, 3, 0))
    facts = [behind[d] for part in order for d in part]
    facts = jnp.stack(facts + [ahead[d] for part in sends for d in part]).astype(jnp.int32)
    place = jnp.concatenate([jnp.stack([row, core]).astype(jnp.int32), slot_count[0]])
    core = core.astype(jnp.int32).reshape(1)
    flat_grad = pooled_grad.reshape(-1, feature)
    keys, targets = lane_view(slot_source), lane_view(slot_target)

    rows = tables * rows_dev
    first, wide, held, keys = first_pick(2, rows, place, keys, targets, flat_grad)
    picked = {2: first}
    picked.update(zip((1, 3), pick_rows((1, 3), place, keys, held, wide)))
    grads = []
    for hop, block in picked.items():
        grads.append(shift(block, "rows", hop))
    begun = own_rows(place, keys, held, wide, rows)
    mine, other = scatter_add(place, begun, grads)
    fetched = fetch(facts, len(order[0]), len(hops), table_rows, begun)
    got = shift(other, "core", 1)
    parts = [None] * len(hops)
    offset = len(hops)
    for part in sends:
        coded = encode_sum(offset, len(part), facts, mine, got, pairs * rings)
        offset += len(part)
        for d, block in zip(part, coded):
            parts[d] = square_shift(block, *hops[d]) if d else block
    parts = lax.all_to_all(first_sum(parts), "far", 0, 0, tiled=True)
    bundle = lax.all_to_all(last_sum(parts), "far", 0, 0, tiled=True)
    whole = [None] * len(hops)
    for d in reversed(range(len(hops))):
        whole[d] = square_shift(bundle, *hops[d]) if d else bundle
    state = keep(accum)
    swapped = [shift(w, "core", 1) for w in whole]
    result = ()
    for i in range(2):
        result = update(
            i * len(order[0]),
            facts,
            core,
            [whole[d] for d in order[i]],
            [swapped[d] for d in order[i]],
            fetched[i],
            state,
            result,
        )
    return result


def solution(mesh):
    split = Mesh(mesh.devices.reshape(4, 2, 4, 2, mesh.shape["rows"]), AXES)
    placed = (
        P(AXES, None, None),
        P(AXES, None, None),
        P(AXES, None, None),
        P(AXES, None),
        P(None, "rows", None),
        P(None, "rows"),
    )

    return jax.shard_map(
        shards,
        mesh=split,
        in_specs=placed,
        out_specs=(P(None, "rows", None), P(None, "rows")),
        check_vma=False,
    )
```

```python
import functools

import jax
import jax.numpy as jnp
from jax import lax
from jax.experimental import pallas as pl
from jax.experimental.pallas import tpu as pltpu
from jax.sharding import Mesh
from jax.sharding import PartitionSpec as P


AXES = ("far", "pair", "ring", "core", "rows")
SQUARE = ("pair", "ring")

LEARN_RATE = 0.1
EPSILON = 1e-06
LANES = 128
SPARE = 8
CODED = LANES + SPARE
STEPS = 64.0
TOP = 32700.0
TINY = 1e-30
ROUNDER = 12582912.0

VM = pl.BlockSpec(memory_space=pltpu.VMEM)
SM = pl.BlockSpec(memory_space=pltpu.SMEM)
HB = pl.BlockSpec(memory_space=pltpu.HBM)


def room(mib):
    return pltpu.CompilerParams(vmem_limit_bytes=mib * 2**20)


def cost(flops):
    return pl.CostEstimate(flops=flops, bytes_accessed=10**6, transcendentals=0)


def loop(count, body):
    def step(i, carry):
        body(i)
        return carry

    lax.fori_loop(0, count, step, 0)


def pieces(count, size, body):
    loop(count // size, lambda i: body(pl.ds(pl.multiple_of(i * size, size), size)))


def pick(owner, keys, held, wide, out, stage):
    chunks = keys.shape[0]
    cap = chunks * LANES

    def body(chunk):
        first = chunk * LANES
        for u in range(LANES):
            key = keys[chunk, owner, u]
            stage[pl.ds(first + u, 1), :] = wide[pl.ds(key, 1), :]

    loop(chunks, body)

    def narrow(rows):
        out[rows, :] = stage[rows, :].astype(jnp.bfloat16)

    pieces(cap, LANES, narrow)
    target = held[owner]
    upper = target >> 7
    out[cap : cap + SPARE, :] = upper.astype(jnp.float32).astype(jnp.bfloat16)
    lower = target - upper * LANES
    out[cap + SPARE : cap + 2 * SPARE, :] = lower.astype(jnp.float32).astype(jnp.bfloat16)


def first_pick_kernel(
    hop, unused, place, keys, keys_in, targets, flat, out, wide, held, kept, stage
):
    chunks, owners, _ = targets.shape
    slots = lax.broadcasted_iota(jnp.int32, (chunks, LANES), 0) * LANES
    slots = slots + lax.broadcasted_iota(jnp.int32, (chunks, LANES), 1)
    kept[...] = keys_in[...]
    for owner in range(owners):
        held[owner] = jnp.where(slots < place[2 + owner], targets[:, owner, :], unused)

    def widen(rows):
        wide[rows, :] = flat[rows, :].astype(jnp.float32)

    pieces(flat.shape[0], LANES, widen)
    pick(lax.rem(place[0] + hop, owners), keys, held, wide, out, stage)


def first_pick(hop, unused, place, keys, targets, flat):
    chunks, owners, _ = keys.shape
    cap = chunks * LANES
    width = flat.shape[1]
    return pl.pallas_call(
        functools.partial(first_pick_kernel, hop, unused),
        out_shape=(
            jax.ShapeDtypeStruct((cap + 2 * SPARE, width), jnp.bfloat16),
            jax.ShapeDtypeStruct(flat.shape, jnp.float32),
            jax.ShapeDtypeStruct((owners, chunks, LANES), jnp.int32),
            jax.ShapeDtypeStruct(keys.shape, jnp.int32),
        ),
        in_specs=[SM, SM, VM, VM, VM],
        out_specs=(VM, VM, VM, VM),
        scratch_shapes=[pltpu.VMEM((cap, width), jnp.float32)],
        compiler_params=room(6),
        cost_estimate=cost(10**7),
        name="first_pick",
    )(place, keys, keys, targets, flat)


def pick_kernel(hops, place, keys, held, wide, *refs):
    outs, stages = refs[: len(hops)], refs[len(hops) :]
    owners = held.shape[0]
    for hop, out, stage in zip(hops, outs, stages):
        pick(lax.rem(place[0] + hop, owners), keys, held, wide, out, stage)


def pick_rows(hops, place, keys, held, wide):
    cap = keys.shape[0] * LANES
    width = wide.shape[1]
    shape = jax.ShapeDtypeStruct((cap + 2 * SPARE, width), jnp.bfloat16)
    return pl.pallas_call(
        functools.partial(pick_kernel, hops),
        out_shape=(shape,) * len(hops),
        in_specs=[SM, SM, VM, VM],
        out_specs=(VM,) * len(hops),
        scratch_shapes=[pltpu.VMEM((cap, width), jnp.float32)] * len(hops),
        compiler_params=room(6),
        cost_estimate=cost(10**7 * len(hops)),
        name="pick",
    )(place, keys, held, wide)


def add_rows(pairs, sums, wides, keys, rows, chunk):
    first = chunk * LANES
    for u in range(0, LANES, 2 * pairs):
        for k, row in enumerate(rows):
            for p in range(pairs):
                at, total = u + 2 * p, sums[k * pairs + p]
                one, two = keys[row + chunk, at], keys[row + chunk, at + 1]
                here, next_ = pl.ds(one, 1), pl.ds(two, 1)
                again = jnp.where(one == two, 1.0, 0.0)
                lead = wides[k][pl.ds(first + at, 1), :]
                tail = wides[k][pl.ds(first + at + 1, 1), :] + lead * again
                before, after = total[here, :], total[next_, :]
                total[here, :] = before + lead
                total[next_, :] = after + tail


def prepare(grads, cap, sums, wides, found, keys, sem):
    chunks = cap // LANES
    for k, grad in enumerate(grads):
        upper = grad[cap : cap + SPARE, :].astype(jnp.float32)
        lower = grad[cap + SPARE : cap + 2 * SPARE, :].astype(jnp.float32)
        found[k * chunks : (k + 1) * chunks, :] = (upper * LANES + lower).astype(jnp.int32)
    copy = pltpu.make_async_copy(found, keys, sem)
    copy.start()

    def widen(rows):
        for wide, grad in zip(wides, grads):
            wide[rows, :] = grad[rows, :].astype(jnp.float32)

    def clear(rows):
        for total in sums:
            total[rows, :] = jnp.zeros((64, LANES), jnp.float32)

    pieces(cap, 64, widen)
    pieces(sums[0].shape[0] // 64 * 64, 64, clear)
    copy.wait()


def own_kernel(parts, place, keys, held, wide, out, *refs):
    sums, (found, sem) = refs[:parts], refs[parts:]
    owner = place[0]
    copy = pltpu.make_async_copy(held.at[owner], found, sem)
    copy.start()

    def clear(rows):
        for total in sums:
            total[rows, :] = jnp.zeros((64, LANES), jnp.float32)

    pieces(sums[0].shape[0] // 64 * 64, 64, clear)
    copy.wait()

    def body(chunk):
        for u in range(0, LANES, 2 * parts):
            for p, total in enumerate(sums):
                at = u + 2 * p
                one, two = found[chunk, at], found[chunk, at + 1]
                lead = wide[pl.ds(keys[chunk, owner, at], 1), :]
                tail = wide[pl.ds(keys[chunk, owner, at + 1], 1), :]
                tail = tail + lead * jnp.where(one == two, 1.0, 0.0)
                here, next_ = pl.ds(one, 1), pl.ds(two, 1)
                before, after = total[here, :], total[next_, :]
                total[here, :] = before + lead
                total[next_, :] = after + tail

    loop(keys.shape[0], body)

    def add_up(rows):
        total = sums[0][rows, :]
        for part in sums[1:]:
            total = total + part[rows, :]
        out[rows, :] = total

    pieces(out.shape[0], 64, add_up)


def add_half(index, begun, sums, out):
    half = out.shape[0]

    def add_up(i):
        there = pl.ds(pl.multiple_of(index * half + i * 64, 64), 64)
        total = begun[there, :]
        for part in sums:
            total = total + part[there, :]
        out[pl.ds(pl.multiple_of(i * 64, 64), 64), :] = total

    loop(half // 64, add_up)


def scatter_kernel(cap, senders, place, begun, *refs):
    grads, other, refs = refs[:senders], refs[senders], refs[senders + 1 :]
    sums, wides = refs[:senders], refs[senders : 2 * senders]
    found, keys, sem = refs[2 * senders :]
    chunks = cap // LANES
    prepare(grads, cap, sums, wides, found, keys, sem)
    rows = [k * chunks for k in range(senders)]
    loop(chunks, lambda chunk: add_rows(1, sums, wides, keys, rows, chunk))
    add_half(1 - place[1], begun, sums, other)


def half_kernel(place, begun, *refs):
    add_half(place[1], begun, refs[:-1], refs[-1])


def tables_of(rows, width, cap, senders, pairs):
    chunks = cap // LANES
    return (
        [pltpu.VMEM((rows + SPARE, width), jnp.float32)] * (senders * pairs)
        + [pltpu.VMEM((cap, width), jnp.float32)] * senders
        + [
            pltpu.VMEM((senders * chunks, LANES), jnp.int32),
            pltpu.SMEM((senders * chunks, LANES), jnp.int32),
            pltpu.SemaphoreType.DMA,
        ]
    )


def own_rows(place, keys, held, wide, rows):
    width = wide.shape[1]
    parts = 2
    return pl.pallas_call(
        functools.partial(own_kernel, parts),
        out_shape=jax.ShapeDtypeStruct((rows, width), jnp.float32),
        in_specs=[SM, SM, VM, VM],
        out_specs=VM,
        scratch_shapes=[pltpu.VMEM((rows + SPARE, width), jnp.float32)] * parts
        + [pltpu.SMEM(held.shape[1:], jnp.int32), pltpu.SemaphoreType.DMA],
        compiler_params=room(16),
        cost_estimate=cost(10**7),
        name="own_rows",
    )(place, keys, held, wide)


def scatter_add(place, begun, grads):
    senders = len(grads)
    cap, width = grads[0].shape[0] - 2 * SPARE, grads[0].shape[1]
    rows = begun.shape[0]
    other = jax.ShapeDtypeStruct((rows // 2, width), jnp.float32)
    table = jax.ShapeDtypeStruct((rows + SPARE, width), jnp.float32)
    other, *sums = pl.pallas_call(
        functools.partial(scatter_kernel, cap, senders),
        out_shape=(other,) + (table,) * senders,
        in_specs=[SM, VM] + [VM] * senders,
        out_specs=(VM,) * (senders + 1),
        scratch_shapes=tables_of(rows, width, cap, senders, 1)[senders:],
        compiler_params=room(8),
        cost_estimate=cost(10**8),
        name="scatter",
    )(place, begun, *grads)
    return other, sums


def sum_half(place, begun, sums):
    rows, width = begun.shape
    return pl.pallas_call(
        half_kernel,
        out_shape=jax.ShapeDtypeStruct((rows // 2, width), jnp.float32),
        in_specs=[SM, VM] + [VM] * len(sums),
        out_specs=VM,
        compiler_params=room(8),
        cost_estimate=cost(10**6),
        name="half",
    )(place, begun, *sums)


def diagonal():
    lane = lax.broadcasted_iota(jnp.int32, (LANES, LANES), 1)
    return lax.broadcasted_iota(jnp.int32, (LANES, LANES), 0) == lane


def to_row(column, diag):
    return jnp.sum(jnp.where(diag, column, 0.0), axis=0, keepdims=True)


def to_column(row, diag):
    return jnp.sum(jnp.where(diag, row, 0.0), axis=1, keepdims=True)


def powers_of(peaks):
    return jnp.ceil(STEPS * jnp.log2(jnp.maximum(peaks, TINY) / TOP))


def short(x):
    return x.astype(jnp.int32).astype(jnp.int16)


def wide_of(x):
    return x.astype(jnp.int32).astype(jnp.float32)


def rounded(x):
    return short((x + ROUNDER) - ROUNDER)


def encode_blocks(block, put, count, peaks, shrinks, diag):
    for k in range(count):
        peak = jnp.max(jnp.abs(block(k)), axis=1, keepdims=True)
        peaks[k : k + 1, :] = to_row(peak, diag)
    powers = powers_of(peaks[...])
    peaks[...] = powers
    shrinks[...] = jnp.exp2(powers * (-1.0 / STEPS))
    for k in range(count):
        tail = short(jnp.broadcast_to(peaks[k : k + 1, :], (SPARE, LANES)))
        put(k, rounded(block(k) * to_column(shrinks[k : k + 1, :], diag)), tail)


def decode(part, diag):
    scale = to_column(jnp.exp2(wide_of(part[LANES:CODED]) * (1.0 / STEPS))[0:1], diag)
    return wide_of(part[0:LANES]) * scale


def encode_kernel(offset, targets, mine, got, *refs):
    outs, (peaks, shrinks) = refs[:-2], refs[-2:]
    diag = diagonal()
    blocks = outs[0].shape[0]
    together = peaks.shape[0] // blocks
    size = blocks * LANES
    for low in range(0, len(outs), together):
        some = outs[low : low + together]

        def block(i, low=low):
            first = targets[offset + low + i // blocks] * size + i % blocks * LANES
            rows = pl.ds(pl.multiple_of(first, LANES), LANES)
            return mine[rows, :] + got[rows, :]

        def put(i, code, tail, some=some):
            out, k = some[i // blocks], i % blocks
            out[k, 0:LANES, :] = code
            out[k, LANES:CODED, :] = tail

        encode_blocks(block, put, len(some) * blocks, peaks, shrinks, diag)


def encode_sum(offset, count, targets, mine, got, groups):
    blocks = mine.shape[0] // (groups * LANES)
    shape = jax.ShapeDtypeStruct((blocks, CODED, LANES), jnp.int16)
    return pl.pallas_call(
        functools.partial(encode_kernel, offset),
        out_shape=(shape,) * count,
        in_specs=[SM, VM, VM],
        out_specs=(VM,) * count,
        scratch_shapes=[pltpu.VMEM((2 * blocks, LANES), jnp.float32)] * 2,
        compiler_params=room(8),
        cost_estimate=cost(10**7),
        name="encode",
    )(targets, mine, got)


def first_sum_kernel(*refs):
    parts, (out, totals, peaks, shrinks) = refs[:-4], refs[-4:]
    diag = diagonal()
    blocks = out.shape[0]

    def body(k, carry):
        total = decode(parts[0][k], diag)
        for part in parts[1:]:
            total = total + decode(part[k], diag)
        totals[k] = total
        return carry

    lax.fori_loop(0, blocks, body, 0)

    def put(k, code, tail):
        out[k, 0:LANES, :] = code
        out[k, LANES:CODED, :] = tail

    encode_blocks(lambda k: totals[k], put, blocks, peaks, shrinks, diag)


def first_sum(parts):
    blocks = parts[0].shape[0]
    return pl.pallas_call(
        first_sum_kernel,
        out_shape=jax.ShapeDtypeStruct(parts[0].shape, jnp.int16),
        in_specs=[VM] * len(parts),
        out_specs=VM,
        scratch_shapes=[pltpu.VMEM((blocks, LANES, LANES), jnp.float32)]
        + [pltpu.VMEM((blocks, LANES), jnp.float32)] * 2,
        compiler_params=room(6),
        cost_estimate=cost(10**7),
        name="first_sum",
    )(*parts)


def last_sum_kernel(parts, out):
    diag = diagonal()
    total = decode(parts[0], diag)
    for j in range(1, parts.shape[0]):
        total = total + decode(parts[j], diag)
    powers = powers_of(to_row(jnp.max(jnp.abs(total), axis=1, keepdims=True), diag))
    code = rounded(total * to_column(jnp.exp2(powers * (-1.0 / STEPS)), diag))
    tail = short(jnp.broadcast_to(powers, (SPARE, LANES)))
    for j in range(out.shape[0]):
        out[j, 0:LANES, :] = code
        out[j, LANES:CODED, :] = tail


def last_sum(parts):
    return pl.pallas_call(
        last_sum_kernel,
        out_shape=jax.ShapeDtypeStruct(parts.shape, jnp.int16),
        in_specs=[VM],
        out_specs=VM,
        compiler_params=room(4),
        cost_estimate=cost(10**6),
        name="last_sum",
    )(parts)


def update_kernel(count, offset, groups, core, *refs):
    mine, got = refs[:count], refs[count : 2 * count]
    rows, state = refs[2 * count : 2 * count + 2]
    new_rows, new_state, held, sums, scales = refs[-5:]
    step = pl.program_id(0)
    tables, blocks = held.shape[:2]
    size = blocks * LANES
    for d in range(count):

        @pl.when(step == d)
        def _():
            held[core[0]] = mine[d][...]
            held[1 - core[0]] = got[d][...]

    diag = diagonal()
    start = groups[offset + step] * size
    every = [(table, k) for table in range(tables) for k in range(blocks)]
    for at, (table, k) in enumerate(every):
        code = wide_of(held[table, k, 0:LANES, :])
        sums[at : at + 1, :] = to_row(jnp.sum(code * code, axis=1, keepdims=True), diag)
        scales[at : at + 1, :] = wide_of(held[table, k, LANES:CODED, :])[0:1]
    scale = jnp.exp2(scales[...] * (1.0 / STEPS))
    gain = sums[...] * (scale * scale) * (1.0 / LANES)
    for at, (table, k) in enumerate(every):
        lanes = slice(k * LANES, (k + 1) * LANES)
        there = pl.ds(pl.multiple_of(start + k * LANES, LANES), LANES)
        updated = state[table : table + 1, there] + gain[at : at + 1, :]
        new_state[table : table + 1, lanes] = updated
        sums[at : at + 1, :] = updated
    scales[...] = LEARN_RATE * scale / (jnp.sqrt(sums[...]) + EPSILON)
    for at, (table, k) in enumerate(every):
        there = slice(k * LANES, (k + 1) * LANES)
        move = wide_of(held[table, k, 0:LANES, :]) * to_column(scales[at : at + 1, :], diag)
        new_rows[table, there, :] = rows[step, table, there, :] - move


def update(offset, groups, core, mine, got, rows, state, earlier):
    count, tables, size, width = rows.shape
    blocks = mine[0].shape[0]
    row_spec = pl.BlockSpec((tables, size, width), lambda i, g, c: (0, g[offset + i], 0))
    state_spec = pl.BlockSpec((tables, size), lambda i, g, c: (0, g[offset + i]))
    first = 2 + 2 * count + 2
    return pl.pallas_call(
        functools.partial(update_kernel, count, offset),
        grid_spec=pltpu.PrefetchScalarGridSpec(
            num_scalar_prefetch=2,
            grid=(count,),
            in_specs=[VM] * (2 * count) + [VM, VM] + [HB] * len(earlier),
            out_specs=(row_spec, state_spec),
            scratch_shapes=[
                pltpu.VMEM((tables, *mine[0].shape), jnp.int16),
            ]
            + [pltpu.VMEM((tables * blocks, LANES), jnp.float32)] * 2,
        ),
        out_shape=(
            jax.ShapeDtypeStruct((tables, state.shape[1], width), jnp.float32),
            jax.ShapeDtypeStruct(state.shape, jnp.float32),
        ),
        input_output_aliases={first: 0, first + 1: 1} if earlier else {},
        compiler_params=room(12),
        cost_estimate=cost(10**7),
        name="update",
    )(groups, core, *mine, *got, rows, state, *earlier)


def fetch_kernel(groups, rows, after, *refs):
    outs, sems = refs[:-1], refs[-1]
    size = outs[0].shape[2]
    copies = []
    for out in outs:
        for d in range(out.shape[0]):
            at = len(copies)
            there = pl.ds(pl.multiple_of(groups[at] * size, size), size)
            copies.append(pltpu.make_async_copy(rows.at[:, there, :], out.at[d], sems.at[at]))
    for copy in copies:
        copy.start()
    for copy in copies:
        copy.wait()


def fetch(groups, split, count, rows, after):
    tables, rows_dev, width = rows.shape
    shapes = [
        jax.ShapeDtypeStruct((size, tables, rows_dev // count, width), rows.dtype)
        for size in (split, count - split)
    ]
    return pl.pallas_call(
        fetch_kernel,
        out_shape=shapes,
        in_specs=[SM, HB, HB],
        out_specs=(VM, VM),
        scratch_shapes=[pltpu.SemaphoreType.DMA((count,))],
        compiler_params=room(5),
        cost_estimate=cost(3 * 10**7),
        name="fetch",
    )(groups, rows, after)


def keep_kernel(state, out):
    out[...] = state[...]


def keep(state):
    return pl.pallas_call(
        keep_kernel,
        out_shape=jax.ShapeDtypeStruct(state.shape, state.dtype),
        in_specs=[VM],
        out_specs=VM,
        compiler_params=room(1),
        cost_estimate=cost(10**5),
        name="keep",
    )(state)


def shift(x, axis, by):
    count = lax.axis_size(axis)
    return lax.ppermute(x, axis, [(i, (i + by) % count) for i in range(count)])


def square_shift(x, pair_by, ring_by):
    pairs, rings = lax.axis_size("pair"), lax.axis_size("ring")
    links = [
        (p * rings + r, (p + pair_by) % pairs * rings + (r + ring_by) % rings)
        for p in range(pairs)
        for r in range(rings)
    ]
    return lax.ppermute(x, SQUARE, links)


def lane_view(slots):
    owners, cap = slots.shape[1:]
    return slots.reshape(owners, cap // LANES, LANES).transpose(1, 0, 2)


def shards(pooled_grad, slot_source, slot_target, slot_count, table_rows, accum):
    feature = pooled_grad.shape[2]
    tables, rows_dev, _ = table_rows.shape
    pairs, rings = lax.axis_size("pair"), lax.axis_size("ring")
    row, core, pair, ring = (lax.axis_index(a) for a in ("rows", "core", "pair", "ring"))
    hops = [(0, 0), (0, 1), (0, 3), (1, 0), (1, 1), (1, 3), (0, 2), (1, 2)]
    behind = [(pair + p) % pairs * rings + (ring + rings - r) % rings for p, r in hops]
    ahead = [(pair + p) % pairs * rings + (ring + r) % rings for p, r in hops]
    order = ((7, 6, 5, 2, 1, 0), (4, 3))
    sends = ((7, 6, 5), (2, 1, 4, 3, 0))
    facts = [behind[d] for part in order for d in part]
    facts = jnp.stack(facts + [ahead[d] for part in sends for d in part]).astype(jnp.int32)
    place = jnp.concatenate([jnp.stack([row, core]).astype(jnp.int32), slot_count[0]])
    core = core.astype(jnp.int32).reshape(1)
    flat_grad = pooled_grad.reshape(-1, feature)
    keys, targets = lane_view(slot_source), lane_view(slot_target)

    rows = tables * rows_dev
    first, wide, held, keys = first_pick(2, rows, place, keys, targets, flat_grad)
    picked = {2: first}
    picked.update(zip((1, 3), pick_rows((1, 3), place, keys, held, wide)))
    grads = []
    for hop, block in picked.items():
        grads.append(shift(block, "rows", hop))
    begun = own_rows(place, keys, held, wide, rows)
    other, sums = scatter_add(place, begun, grads)
    mine = sum_half(place, begun, sums)
    fetched = fetch(facts, len(order[0]), len(hops), table_rows, begun)
    got = shift(other, "core", 1)
    parts = [None] * len(hops)
    offset = len(hops)
    for part in sends:
        coded = encode_sum(offset, len(part), facts, mine, got, pairs * rings)
        offset += len(part)
        for d, block in zip(part, coded):
            parts[d] = square_shift(block, *hops[d]) if d else block
    parts = lax.all_to_all(first_sum(parts), "far", 0, 0, tiled=True)
    bundle = lax.all_to_all(last_sum(parts), "far", 0, 0, tiled=True)
    whole = [None] * len(hops)
    for d in reversed(range(len(hops))):
        whole[d] = square_shift(bundle, *hops[d]) if d else bundle
    state = keep(accum)
    swapped = [shift(w, "core", 1) for w in whole]
    result = ()
    for i in range(2):
        result = update(
            i * len(order[0]),
            facts,
            core,
            [whole[d] for d in order[i]],
            [swapped[d] for d in order[i]],
            fetched[i],
            state,
            result,
        )
    return result


def solution(mesh):
    split = Mesh(mesh.devices.reshape(4, 2, 4, 2, mesh.shape["rows"]), AXES)
    placed = (
        P(AXES, None, None),
        P(AXES, None, None),
        P(AXES, None, None),
        P(AXES, None),
        P(None, "rows", None),
        P(None, "rows"),
    )

    return jax.shard_map(
        shards,
        mesh=split,
        in_specs=placed,
        out_specs=(P(None, "rows", None), P(None, "rows")),
        check_vma=False,
    )
```
